128 devices in a mesh: lat: 16 (over x, z_lo, core), lon: 8 (over z_hi, y).
Axes of the slice: x: 4, y: 4, z: 4 (z_hi: 2, z_lo: 2; z = z_hi * 2 + z_lo), core: 2. Of those that a mesh axis runs over, the one named last changes fastest.
Arguments:
- current: bfloat16 [69, 512, 1024], P(None, 'lat', 'lon')
- next_fields: bfloat16 [128, 512, 1024], P(('lat', 'lon')), may hold values from -6 to 6
- reader_slot: int32 [69], replicated, may hold values from 0 to 127, as said below
- first_weight: bfloat16 [9, 256, 69], replicated, may hold values from -0.25 to 0.25
- first_bias: float32 [256], replicated, may hold values from -3 to 3
- second_weight: bfloat16 [9, 256, 256], replicated, may hold values from -0.125 to 0.125
- second_bias: float32 [256], replicated, may hold values from -3 to 3
Outputs:
- features: bfloat16 [256, 512, 1024], P(None, 'lat', 'lon')
- next_tile: bfloat16 [69, 512, 1024], P(None, 'lat', 'lon')
The draws below stay inside these ranges and needn't reach their ends.
Inputs may be any that keep to these rules, and one draw needn't show every extreme that they name: `reader_slot`: the 69 entries are different slots.
All inputs are finite; a program needn't handle non-finite values.
Results may differ from the reference program's by a relative error of at most 0.0053.
Values may be sent and summed in bfloat16 or wider, within the bound.
No kernel may reach another device: no remote copies, remote signals or barrier semaphores. Data moves between devices by JAX's collectives and lax.ppermute only.
A program may use at most 128 MiB of HBM per device.

```python
import jax
import jax.numpy as jnp
from jax import lax

C = 69
HID = 256
LAT_DEV = 32
LON_DEV = 128
H = 512
W = 1024
SLOTS = 128


def draw_current(key, part):
    keys = jax.random.split(jax.random.fold_in(key, 11), 7)
    profile = (jnp.arange(H, dtype=jnp.float32) / (H - 1))[None, :, None]
    rough = jax.random.uniform(keys[4], (C, 1, W), jnp.float32, 0.5, 1.5)
    slope = jax.random.uniform(keys[2], (C, 1, 1), jnp.float32, -2.0, 2.0)
    lat_tiles = H // LAT_DEV
    lon_tiles = W // LON_DEV
    tile_level = jax.random.normal(keys[5], (C, lat_tiles, 1, lon_tiles, 1), jnp.float32)
    tile_field = jnp.broadcast_to(tile_level, (C, lat_tiles, LAT_DEV, lon_tiles, LON_DEV)).reshape(C, H, W)
    half_level = jax.random.normal(keys[6], (C, 1, 2), jnp.float32)
    half_field = jnp.repeat(half_level, W // 2, axis=2)
    noise = jax.random.normal(keys[0], (C, H, W), jnp.float32)
    offset = jax.random.normal(keys[1], (C, 1, 1), jnp.float32)
    spread = 1.0 + 2.0 * profile
    tile_scale = 0.8
    values = offset + 3.0 * slope * profile + tile_scale * tile_field + half_field + spread * rough * noise
    return values.astype(jnp.bfloat16)


def draw_reader_slot(key, part):
    order = jax.random.permutation(jax.random.fold_in(key, 23), SLOTS)
    return order[:C].astype(jnp.int32)


def steps_of(rng, shape, shards, smallest, top_value):
    loudness = 1.0
    for dim, shards_of in shards:
        heights = jax.random.uniform(jax.random.fold_in(jax.random.fold_in(rng, 6), dim), (shards_of,), jnp.float32, smallest / len(shards), top_value / len(shards))
        loudness = loudness * jnp.repeat(jnp.exp(heights), shape[dim] // shards_of).reshape((-1,) + (1,) * (len(shape) - 1 - dim))
    return loudness


def scatter_about(own_key, dims, scale, most, cuts=(), held_as=jnp.bfloat16):
    level = steps_of(own_key, dims, cuts, -0.22, 0.18) if cuts else 1.0
    drawn = jax.random.normal(own_key, dims, jnp.float32) * scale * level
    return jnp.minimum(jnp.maximum(drawn, -most), most).astype(held_as)


def setup_inputs(seed: int = 0) -> dict:
    key_of = jax.random.split(jax.random.key(seed), 8)
    current = draw_current(jax.random.fold_in(key_of[7], 71), 0)
    next_fields = scatter_about(key_of[1], (SLOTS, H, W), 1.0, 6.0, ((0, 128),))
    reader_slot = draw_reader_slot(jax.random.fold_in(key_of[7], 71), 0)
    first_weight = scatter_about(key_of[3], (9, HID, C), (9 * C) ** -0.5, 0.25)
    first_bias = scatter_about(key_of[4], (HID,), 0.5, 3.0, (), jnp.float32)
    second_weight = scatter_about(key_of[5], (9, HID, HID), (9 * HID) ** -0.5, 0.125)
    second_bias = scatter_about(key_of[6], (HID,), 0.5, 3.0, (), jnp.float32)
    return {"current": current, "next_fields": next_fields, "reader_slot": reader_slot, "first_weight": first_weight, "first_bias": first_bias, "second_weight": second_weight, "second_bias": second_bias}


def conv_grid(field, weight):
    padded = jnp.pad(field.astype(jnp.float32), ((0, 0), (1, 1), (0, 0)))
    padded = jnp.concatenate([padded[:, :, -1:], padded, padded[:, :, :1]], axis=2)
    rows = field.shape[1]
    cols = field.shape[2]
    total = jnp.zeros((weight.shape[1], rows, cols), jnp.float32)
    for tap in range(9):
        shifted = padded[:, tap // 3:tap // 3 + rows, tap % 3:tap % 3 + cols]
        total = total + jnp.einsum('ok,khw->ohw', weight[tap].astype(jnp.float32), shifted)
    return total

def reference(current, next_fields, reader_slot, first_weight, first_bias, second_weight, second_bias):
    values = current.astype(jnp.float32)
    cells = values.shape[1] * values.shape[2]
    mean = lax.optimization_barrier(jnp.sum(values, axis=(1, 2))) / cells
    square = lax.optimization_barrier(jnp.sum(values * values, axis=(1, 2))) / cells
    scale = 1.0 / jnp.sqrt(square - mean * mean + 1e-05)
    normed = ((values - mean[:, None, None]) * scale[:, None, None]).astype(jnp.bfloat16)
    hidden = jax.nn.gelu(conv_grid(normed, first_weight) + first_bias[:, None, None], approximate=True).astype(jnp.bfloat16)
    features = (conv_grid(hidden, second_weight) + second_bias[:, None, None]).astype(jnp.bfloat16)
    next_tile = jnp.take(next_fields, reader_slot, axis=0)
    return (features, next_tile)
```

```python
import functools

import jax
import jax.numpy as jnp
from jax import lax
from jax.experimental import pallas as pl
from jax.experimental.pallas import tpu as pltpu
from jax.sharding import Mesh
from jax.sharding import PartitionSpec as P

LAT = ("lat_0", "lat_1", "lat_2")
LON = ("lon_0", "lon_1")
LANES = 128
BLOCK = 8
GELU_C = 0.7978845608028654


def gelu(v):
    return (0.5 * v) * (1.0 + jnp.tanh(v * (GELU_C + (GELU_C * 0.044715) * (v * v))))


def conv_kernel(
    channels, rows, cols, hid,
    ends_ref, x_ref, top_ref, bottom_ref, left_ref, right_ref, edge_ref, mean_ref, scale_ref,
    w1_ref, b1_ref, w2_ref, b2_ref, out_ref,
    taps_ref, edge_taps_ref, edge_hid_ref, west_ref, mid_ref, east_ref, turned_ref,
):
    mean = mean_ref[...]
    scale = scale_ref[...]
    first = ends_ref[0] != 0
    last = ends_ref[1] != 0
    lane = lax.broadcasted_iota(jnp.int32, (cols, LANES), 1)
    sub = lax.broadcasted_iota(jnp.int32, (cols, LANES), 0)
    sub_hid = lax.broadcasted_iota(jnp.int32, (cols, hid), 0)
    over = 2 * channels - LANES

    def norm(raw):
        return (raw.astype(jnp.float32) - mean) * scale

    def pack(minus, zero, plus, lanes):
        turned = pltpu.roll(zero, channels, axis=1)
        low = jnp.where(lanes < channels, minus, turned)
        high = jnp.where(lanes < over, turned, pltpu.roll(plus, over, axis=1))
        return low, high

    def build(raw, row, keep):
        main = norm(raw)
        left = norm(left_ref[row])
        right = norm(right_ref[row])
        if keep is not None:
            main = jnp.where(keep, main, 0.0)
            left = jnp.where(keep, left, 0.0)
            right = jnp.where(keep, right, 0.0)
        minus = jnp.where(sub == 0, left[1:2], pltpu.roll(main, 1, axis=0))
        plus = jnp.where(sub == cols - 1, right[0:1], pltpu.roll(main, cols - 1, axis=0))
        low, high = pack(minus, main, plus, lane)
        taps_ref[row, :, 0:LANES] = low.astype(jnp.bfloat16)
        taps_ref[row, :, LANES : 2 * LANES] = high.astype(jnp.bfloat16)

    for r in range(2):
        build(top_ref[r], r, jnp.logical_not(first))
        build(bottom_ref[r], rows + 2 + r, jnp.logical_not(last))

    @pl.loop(0, rows)
    def _(r):
        build(x_ref[r], r + 2, None)

    tall = edge_ref.shape[2]
    edge_row = lax.broadcasted_iota(jnp.int32, (tall, LANES), 0)
    edge_lane = lax.broadcasted_iota(jnp.int32, (tall, LANES), 1)
    outside = jnp.logical_or(
        jnp.logical_and(first, edge_row < 2), jnp.logical_and(last, edge_row >= rows + 2)
    )
    hid_row = lax.broadcasted_iota(jnp.int32, (tall - 8, hid), 0)
    hid_outside = jnp.logical_or(
        jnp.logical_and(first, hid_row < 1), jnp.logical_and(last, hid_row >= rows + 1)
    )
    for side in range(2):
        parts = [jnp.where(outside, 0.0, norm(edge_ref[side, b])) for b in range(3)]
        low, high = pack(*parts, edge_lane)
        edge_taps_ref[:, 0:LANES] = low
        edge_taps_ref[:, LANES : 2 * LANES] = high
        stacked = jnp.concatenate(
            [edge_taps_ref[a : a + tall - 8, :].astype(jnp.bfloat16) for a in range(3)], axis=1
        )
        value = jnp.dot(stacked, w1_ref[...], preferred_element_type=jnp.float32) + b1_ref[...]
        edge_hid_ref[side] = jnp.where(hid_outside, 0.0, gelu(value))

    def hidden(row, count, keep):
        stacked = jnp.concatenate(
            [taps_ref[pl.ds(row + a, count)].reshape(count * cols, 2 * LANES) for a in range(3)], axis=1
        )
        value = jnp.dot(stacked, w1_ref[...], preferred_element_type=jnp.float32) + b1_ref[...]
        value = gelu(value)
        for i in range(count):
            one = value[i * cols : (i + 1) * cols]
            if keep is not None:
                one = jnp.where(keep, one, 0.0)
            west = jnp.where(sub_hid == 0, edge_hid_ref[0, pl.ds(row + i, 1), :], pltpu.roll(one, 1, axis=0))
            east = jnp.where(
                sub_hid == cols - 1, edge_hid_ref[1, pl.ds(row + i, 1), :], pltpu.roll(one, cols - 1, axis=0)
            )
            west_ref[row + i] = west.astype(jnp.bfloat16)
            mid_ref[row + i] = one.astype(jnp.bfloat16)
            east_ref[row + i] = east.astype(jnp.bfloat16)

    hidden(0, 1, jnp.logical_not(first))
    hidden(rows + 1, 1, jnp.logical_not(last))

    @pl.loop(0, rows // 4)
    def _(t):
        hidden(1 + t * 4, 4, None)

    @pl.loop(0, rows // BLOCK)
    def _(t):
        base = t * BLOCK
        stacked = jnp.concatenate(
            [
                ref[pl.ds(base + a, BLOCK)].reshape(BLOCK * cols, hid)
                for a in range(3)
                for ref in (west_ref, mid_ref, east_ref)
            ],
            axis=1,
        )
        value = jnp.dot(stacked, w2_ref[...], preferred_element_type=jnp.float32) + b2_ref[...]
        for i in range(BLOCK):
            turned_ref[pl.ds(i, hid, stride=BLOCK), :] = value[i * cols : (i + 1) * cols].T
        out_ref[:, pl.ds(pl.multiple_of(base, BLOCK), BLOCK), :] = (
            turned_ref[...].reshape(hid, BLOCK, cols).astype(jnp.bfloat16)
        )


def convs(ends, x, top, bottom, left, right, edge, mean, scale, w1, b1, w2, b2):
    rows, cols = x.shape[0], x.shape[1]
    hid = w2.shape[1]
    channels = 69
    tall = edge.shape[2]
    vmem = pl.BlockSpec(memory_space=pltpu.VMEM)
    flops = 2 * hid * (rows * cols * 9 * hid + (rows + 2) * (cols + 2) * 3 * 256)
    return pl.pallas_call(
        functools.partial(conv_kernel, channels, rows, cols, hid),
        out_shape=jax.ShapeDtypeStruct((hid, rows, cols), jnp.bfloat16),
        in_specs=[pl.BlockSpec(memory_space=pltpu.SMEM)] + [vmem] * 12,
        out_specs=vmem,
        scratch_shapes=[
            pltpu.VMEM((rows + 4, cols, 2 * LANES), jnp.bfloat16),
            pltpu.VMEM((tall, 2 * LANES), jnp.float32),
            pltpu.VMEM((2, tall - 8, hid), jnp.float32),
            pltpu.VMEM((rows + 2, cols, hid), jnp.bfloat16),
            pltpu.VMEM((rows + 2, cols, hid), jnp.bfloat16),
            pltpu.VMEM((rows + 2, cols, hid), jnp.bfloat16),
            pltpu.VMEM((hid * BLOCK, cols), jnp.float32),
        ],
        compiler_params=pltpu.CompilerParams(vmem_limit_bytes=48 * 2**20),
        cost_estimate=pl.CostEstimate(flops=flops, bytes_accessed=8 * 2**20, transcendentals=0),
        name="convs",
    )(ends, x, top, bottom, left, right, edge, mean, scale, w1, b1, w2, b2)


def shift_pairs(count, periodic):
    forward = [(i, i + 1) for i in range(count - 1)]
    if periodic:
        forward.append((count - 1, 0))
    return forward, [(b, a) for a, b in forward]


def body(current, next_fields, reader_slot, first_weight, first_bias, second_weight, second_bias):
    channels, rows, cols = current.shape
    hid = first_weight.shape[1]
    n_lat = lax.axis_size(LAT)
    n_lon = lax.axis_size(LON)
    cells = rows * n_lat * cols * n_lon

    values = current.astype(jnp.float32)
    sums = jnp.stack([jnp.sum(values, axis=(1, 2)), jnp.sum(values * values, axis=(1, 2))])
    sums = jnp.pad(sums, ((0, 0), (0, LANES - channels)))
    spread = jnp.broadcast_to(sums[None], (n_lat * n_lon,) + sums.shape)
    gathered = lax.all_to_all(spread, LON + LAT, split_axis=0, concat_axis=0, tiled=True)

    turned = jnp.pad(current.transpose(1, 2, 0), ((0, 0), (0, 0), (0, LANES - channels)))
    forward, backward = shift_pairs(n_lat, False)
    top = lax.ppermute(turned[rows - 2 :], LAT, forward)
    bottom = lax.ppermute(turned[:2], LAT, backward)
    forward, backward = shift_pairs(n_lon, True)

    def tall(low, high):
        return jnp.concatenate([top[:, low:high], turned[:, low:high], bottom[:, low:high]], axis=0)

    first_cols, last_cols = tall(0, 2), tall(cols - 2, cols)
    left = lax.ppermute(last_cols, LON, forward)
    right = lax.ppermute(first_cols, LON, backward)
    edge = jnp.stack([
        jnp.stack([left[:, 0], left[:, 1], first_cols[:, 0]]),
        jnp.stack([last_cols[:, 1], right[:, 0], right[:, 1]]),
    ])
    edge = jnp.pad(edge, ((0, 0), (0, 0), (0, 48 - rows - 4), (0, 0)))

    blocks = next_fields.reshape(rows * n_lat, n_lon, cols).transpose(1, 0, 2)
    blocks = blocks.reshape(n_lon * n_lat, rows, cols)
    moved = lax.all_to_all(blocks, LON + LAT, split_axis=0, concat_axis=0, tiled=True)

    total = jnp.sum(gathered, axis=0)
    mean = total[0] / cells
    scale = 1.0 / jnp.sqrt(total[1] / cells - mean * mean + 1e-05)
    scale = jnp.where(jnp.arange(LANES) < channels, scale, 0.0)

    w1 = first_weight.transpose(0, 2, 1).reshape(3, 3 * channels, hid)
    w1 = jnp.pad(w1, ((0, 0), (0, 2 * LANES - 3 * channels), (0, 0))).reshape(6 * LANES, hid)
    w2 = second_weight.transpose(0, 2, 1).reshape(9 * hid, hid)
    at = lax.axis_index(LAT)
    ends = jnp.stack([at == 0, at == n_lat - 1]).astype(jnp.int32)
    features = convs(
        ends, turned, top, bottom, left, right, edge, mean[None], scale[None],
        w1, first_bias[None], w2, second_bias[None],
    )
    place = (reader_slot % n_lon) * n_lat + reader_slot // n_lon
    next_tile = moved.at[place].get(mode="promise_in_bounds")
    return (features, next_tile)


def solution(mesh):
    split = Mesh(mesh.devices.reshape(4, 2, 2, 2, 4), ("lat_0", "lat_1", "lat_2", "lon_0", "lon_1"))
    return jax.shard_map(
        body,
        mesh=split,
        in_specs=(P(None, LAT, LON), P(LAT + LON, None, None), P(), P(), P(), P(), P()),
        out_specs=(P(None, LAT, LON), P(None, LAT, LON)),
        check_vma=False,
    )
```

```python
import functools

import jax
import jax.numpy as jnp
from jax import lax
from jax.experimental import pallas as pl
from jax.experimental.pallas import tpu as pltpu
from jax.sharding import Mesh
from jax.sharding import PartitionSpec as P

LAT = ("lat_0", "lat_1", "lat_2")
LON = ("lon_0", "lon_1")
LANES = 128
BLOCK = 8
GELU_C = 0.7978845608028654


def gelu(v):
    return (0.5 * v) * (1.0 + jnp.tanh(v * (GELU_C + (GELU_C * 0.044715) * (v * v))))


def conv_kernel(
    channels, rows, cols, hid,
    ends_ref, x_ref, top_ref, bottom_ref, left_ref, right_ref, edge_ref, mean_ref, scale_ref,
    w1_raw_ref, b1_ref, w2_raw_ref, b2_ref, out_ref,
    w1_ref, w2_ref, taps_ref, edge_taps_ref, edge_hid_ref, west_ref, mid_ref, east_ref, turned_ref, done_ref, sem,
):
    mean = mean_ref[...]
    scale = scale_ref[...]
    first = ends_ref[0] != 0
    last = ends_ref[1] != 0
    lane = lax.broadcasted_iota(jnp.int32, (cols, LANES), 1)
    sub = lax.broadcasted_iota(jnp.int32, (8, LANES), 0)
    sub_hid = lax.broadcasted_iota(jnp.int32, (8, hid), 0)
    over = 2 * channels - LANES

    def weights():
        group = w1_raw_ref.shape[1]
        for a in range(3):
            for b in range(3):
                w1_ref[a * 2 * LANES + b * group : a * 2 * LANES + (b + 1) * group, :] = w1_raw_ref[3 * a + b]
            w1_ref[a * 2 * LANES + 3 * group : (a + 1) * 2 * LANES, :] = jnp.zeros(
                (2 * LANES - 3 * group, hid), jnp.bfloat16
            )
        for tap in range(9):
            w2_ref[tap * hid : (tap + 1) * hid, :] = w2_raw_ref[tap].T

    def norm(raw):
        return (raw.astype(jnp.float32) - mean) * scale

    def pack(minus, zero, plus, lanes):
        turned = pltpu.roll(zero, channels, axis=1)
        low = jnp.where(lanes < channels, minus, turned)
        high = jnp.where(lanes < over, turned, pltpu.roll(plus, over, axis=1))
        return low, high

    def shifted(main, before, after, sub8):
        minus = pltpu.roll(main, 1, axis=0)
        minus = jnp.concatenate([jnp.where(sub8 == 0, before, minus[:8]), minus[8:]], axis=0)
        plus = pltpu.roll(main, cols - 1, axis=0)
        plus = jnp.concatenate([plus[: cols - 8], jnp.where(sub8 == 7, after, plus[cols - 8 :])], axis=0)
        return minus, plus

    def build(row):
        if row < 2:
            raw, keep = top_ref[row], jnp.logical_not(first)
        elif row >= rows + 2:
            raw, keep = bottom_ref[row - rows - 2], jnp.logical_not(last)
        else:
            raw, keep = x_ref[row - 2], None
        main = norm(raw)
        left = norm(left_ref[row])
        right = norm(right_ref[row])
        if keep is not None:
            main = jnp.where(keep, main, 0.0)
            left = jnp.where(keep, left, 0.0)
            right = jnp.where(keep, right, 0.0)
        minus, plus = shifted(main, left[1:2], right[0:1], sub)
        low, high = pack(minus, main, plus, lane)
        taps_ref[row, :, 0:LANES] = low.astype(jnp.bfloat16)
        taps_ref[row, :, LANES : 2 * LANES] = high.astype(jnp.bfloat16)

    def edges():
        tall = edge_ref.shape[2]
        edge_row = lax.broadcasted_iota(jnp.int32, (tall, LANES), 0)
        edge_lane = lax.broadcasted_iota(jnp.int32, (tall, LANES), 1)
        outside = jnp.logical_or(
            jnp.logical_and(first, edge_row < 2), jnp.logical_and(last, edge_row >= rows + 2)
        )
        hid_row = lax.broadcasted_iota(jnp.int32, (tall - 8, hid), 0)
        hid_outside = jnp.logical_or(
            jnp.logical_and(first, hid_row < 1), jnp.logical_and(last, hid_row >= rows + 1)
        )
        for side in range(2):
            parts = [jnp.where(outside, 0.0, norm(edge_ref[side, b])) for b in range(3)]
            low, high = pack(*parts, edge_lane)
            edge_taps_ref[side, :, 0:LANES] = low
            edge_taps_ref[side, :, LANES : 2 * LANES] = high
            stacked = jnp.concatenate(
                [edge_taps_ref[side, a : a + tall - 8, :].astype(jnp.bfloat16) for a in range(3)], axis=1
            )
            value = jnp.dot(stacked, w1_ref[...], preferred_element_type=jnp.float32) + b1_ref[...]
            edge_hid_ref[side] = jnp.where(hid_outside, 0.0, gelu(value))

    def hidden(row, count):
        stacked = jnp.concatenate(
            [taps_ref[row + a : row + a + count].reshape(count * cols, 2 * LANES) for a in range(3)], axis=1
        )
        value = jnp.dot(stacked, w1_ref[...], preferred_element_type=jnp.float32)
        for i in range(count):
            r = row + i
            one = gelu(value[i * cols : (i + 1) * cols] + b1_ref[...])
            if r == 0:
                one = jnp.where(first, 0.0, one)
            elif r == rows + 1:
                one = jnp.where(last, 0.0, one)
            west, east = shifted(one, edge_hid_ref[0, r : r + 1, :], edge_hid_ref[1, r : r + 1, :], sub_hid)
            west_ref[r] = west.astype(jnp.bfloat16)
            mid_ref[r] = one.astype(jnp.bfloat16)
            east_ref[r] = east.astype(jnp.bfloat16)

    def put(t):
        return pltpu.make_async_copy(
            done_ref.at[t], out_ref.at[:, t * BLOCK : (t + 1) * BLOCK, :], sem.at[t]
        )

    def features(t):
        base = t * BLOCK
        stacked = jnp.concatenate(
            [
                ref[base + a : base + a + BLOCK].reshape(BLOCK * cols, hid)
                for a in range(3)
                for ref in (west_ref, mid_ref, east_ref)
            ],
            axis=1,
        )
        value = jnp.dot(stacked, w2_ref[...], preferred_element_type=jnp.float32) + b2_ref[...]
        for i in range(BLOCK):
            turned_ref[t % 2, pl.ds(i, hid, stride=BLOCK), :] = value[i * cols : (i + 1) * cols].T
        done_ref[t] = turned_ref[t % 2].reshape(hid, BLOCK, cols).astype(jnp.bfloat16)
        put(t).start()

    steps = rows // BLOCK
    weights()
    for r in range(BLOCK + 4):
        build(r)
    edges()
    hidden(0, BLOCK + 2)
    for r in range(BLOCK + 4, 2 * BLOCK + 4):
        build(r)
    for t in range(steps):
        if t + 2 < steps:
            for r in range((t + 2) * BLOCK + 4, (t + 3) * BLOCK + 4):
                build(r)
        if t + 1 < steps:
            hidden((t + 1) * BLOCK + 2, BLOCK)
        features(t)
    for t in range(steps):
        put(t).wait()


def convs(ends, x, top, bottom, left, right, edge, mean, scale, w1, b1, w2, b2):
    rows, cols = x.shape[0], x.shape[1]
    hid = w2.shape[1]
    channels = w1.shape[1]
    tall = edge.shape[2]
    vmem = pl.BlockSpec(memory_space=pltpu.VMEM)
    flops = 2 * hid * (rows * cols * 9 * hid + (rows + 2) * (cols + 2) * 3 * 256)
    return pl.pallas_call(
        functools.partial(conv_kernel, channels, rows, cols, hid),
        out_shape=jax.ShapeDtypeStruct((hid, rows, cols), jnp.bfloat16),
        in_specs=[pl.BlockSpec(memory_space=pltpu.SMEM)] + [vmem] * 12,
        out_specs=pl.BlockSpec(memory_space=pl.ANY),
        scratch_shapes=[
            pltpu.VMEM((6 * LANES, hid), jnp.bfloat16),
            pltpu.VMEM((9 * hid, hid), jnp.bfloat16),
            pltpu.VMEM((rows + 4, cols, 2 * LANES), jnp.bfloat16),
            pltpu.VMEM((2, tall, 2 * LANES), jnp.float32),
            pltpu.VMEM((2, tall - 8, hid), jnp.float32),
            pltpu.VMEM((rows + 2, cols, hid), jnp.bfloat16),
            pltpu.VMEM((rows + 2, cols, hid), jnp.bfloat16),
            pltpu.VMEM((rows + 2, cols, hid), jnp.bfloat16),
            pltpu.VMEM((2, hid * BLOCK, cols), jnp.float32),
            pltpu.VMEM((rows // BLOCK, hid, BLOCK, cols), jnp.bfloat16),
            pltpu.SemaphoreType.DMA((rows // BLOCK,)),
        ],
        compiler_params=pltpu.CompilerParams(vmem_limit_bytes=48 * 2**20),
        cost_estimate=pl.CostEstimate(flops=flops, bytes_accessed=8 * 2**20, transcendentals=0),
        name="convs",
    )(ends, x, top, bottom, left, right, edge, mean, scale, w1, b1, w2, b2)


def prepare_kernel(
    channels, odd_ref, x_ref, fields_ref,
    turned_ref, spread_ref, one_ref, two_ref, west_ref, east_ref, blocks_ref,
    wide_ref, sem,
):
    rows, cols = turned_ref.shape[0], turned_ref.shape[1]
    count = blocks_ref.shape[0]

    def get(j):
        return pltpu.make_async_copy(
            fields_ref.at[0, :, j * cols : (j + 1) * cols], blocks_ref.at[j], sem.at[j]
        )

    for j in range(count):
        get(j).start()
    padded = wide_ref.shape[0] // rows
    wide_ref[0 : channels * rows, :] = x_ref[...].astype(jnp.float32).reshape(channels * rows, cols)
    wide_ref[channels * rows :, :] = jnp.zeros(((padded - channels) * rows, cols), jnp.float32)
    rest = jnp.zeros((LANES - padded, cols), jnp.float32)
    total = jnp.zeros((padded, cols), jnp.float32)
    square = jnp.zeros((padded, cols), jnp.float32)
    for r in range(rows):
        one = wide_ref[pl.ds(r, padded, stride=rows), :]
        total += one
        square += one * one
        turned = jnp.concatenate([one, rest], axis=0).T.astype(jnp.bfloat16)
        turned_ref[r] = turned
        west_ref[r] = turned[:2]
        east_ref[r] = turned[cols - 2 :]
    odd = odd_ref[0] != 0
    low = turned_ref[0:2]
    high = turned_ref[rows - 2 : rows]
    one_ref[...] = jnp.where(odd, low, high)
    two_ref[...] = jnp.where(odd, high, low)

    def sums(value):
        return jnp.sum(jnp.concatenate([value, rest], axis=0).T, axis=0, keepdims=True)

    both = jnp.concatenate([sums(total), sums(square)], axis=0)
    spread_ref[...] = jnp.broadcast_to(both[None], spread_ref.shape)
    for j in range(count):
        get(j).wait()


def prepare(odd, current, next_fields, devices, n_lon):
    channels, rows, cols = current.shape
    vmem = pl.BlockSpec(memory_space=pltpu.VMEM)
    height = next_fields.shape[1]
    padded = (channels + 7) // 8 * 8
    return pl.pallas_call(
        functools.partial(prepare_kernel, channels),
        out_shape=(
            jax.ShapeDtypeStruct((rows, cols, LANES), jnp.bfloat16),
            jax.ShapeDtypeStruct((devices, 2, LANES), jnp.float32),
            jax.ShapeDtypeStruct((2, cols, LANES), jnp.bfloat16),
            jax.ShapeDtypeStruct((2, cols, LANES), jnp.bfloat16),
            jax.ShapeDtypeStruct((rows, 2, LANES), jnp.bfloat16),
            jax.ShapeDtypeStruct((rows, 2, LANES), jnp.bfloat16),
            jax.ShapeDtypeStruct((n_lon, height, cols), jnp.bfloat16),
        ),
        in_specs=[pl.BlockSpec(memory_space=pltpu.SMEM), vmem, pl.BlockSpec(memory_space=pltpu.HBM)],
        out_specs=(vmem,) * 7,
        scratch_shapes=[
            pltpu.VMEM((padded * rows, cols), jnp.float32),
            pltpu.SemaphoreType.DMA((n_lon,)),
        ],
        compiler_params=pltpu.CompilerParams(vmem_limit_bytes=32 * 2**20),
        cost_estimate=pl.CostEstimate(flops=2**24, bytes_accessed=2**22, transcendentals=0),
        name="prepare",
    )(odd, current, next_fields)


def pairs(count, periodic):
    near = [(i, i ^ 1) for i in range(count)]
    far = [(i, i + 1 if i % 2 else i - 1) for i in range(count)]
    if periodic:
        far = [(a, b % count) for a, b in far]
    else:
        far = [(a, b) for a, b in far if 0 <= b < count]
    return near, far


def body(current, next_fields, reader_slot, first_weight, first_bias, second_weight, second_bias):
    channels, rows, cols = current.shape
    n_lat = lax.axis_size(LAT)
    n_lon = lax.axis_size(LON)
    cells = rows * n_lat * cols * n_lon
    at_lat = lax.axis_index(LAT)
    odd_lat = at_lat % 2 == 1
    odd_lon = lax.axis_index(LON) % 2 == 1

    turned, spread, one, two, west, east, blocks = prepare(
        odd_lat.astype(jnp.int32)[None], current, next_fields, n_lat * n_lon, n_lon
    )

    near, far = pairs(n_lat, False)
    one = lax.ppermute(one, LAT, near)
    two = lax.ppermute(two, LAT, far)
    gathered = lax.all_to_all(spread, LON + LAT, split_axis=0, concat_axis=0, tiled=True)
    top = jnp.where(odd_lat, one, two)
    bottom = jnp.where(odd_lat, two, one)
    first_cols = jnp.concatenate([top[:, :2], west, bottom[:, :2]], axis=0)
    last_cols = jnp.concatenate([top[:, cols - 2 :], east, bottom[:, cols - 2 :]], axis=0)
    near, far = pairs(n_lon, True)
    one = lax.ppermute(jnp.where(odd_lon, first_cols, last_cols), LON, near)
    two = lax.ppermute(jnp.where(odd_lon, last_cols, first_cols), LON, far)
    left = jnp.where(odd_lon, one, two)
    right = jnp.where(odd_lon, two, one)
    edge = jnp.stack([
        jnp.stack([left[:, 0], left[:, 1], first_cols[:, 0]]),
        jnp.stack([last_cols[:, 1], right[:, 0], right[:, 1]]),
    ])
    edge = jnp.pad(edge, ((0, 0), (0, 0), (0, 48 - rows - 4), (0, 0)))

    moved = lax.all_to_all(
        blocks.reshape(n_lon * n_lat, rows, cols), LON + LAT, split_axis=0, concat_axis=0, tiled=True
    )

    total = jnp.sum(gathered, axis=0)
    mean = total[0] / cells
    scale = 1.0 / jnp.sqrt(total[1] / cells - mean * mean + 1e-05)
    scale = jnp.where(jnp.arange(LANES) < channels, scale, 0.0)

    w1 = jnp.pad(first_weight.transpose(0, 2, 1), ((0, 0), (0, -channels % 8), (0, 0)))
    ends = jnp.stack([at_lat == 0, at_lat == n_lat - 1]).astype(jnp.int32)
    features = convs(
        ends, turned, top, bottom, left, right, edge, mean[None], scale[None],
        w1, first_bias[None], second_weight, second_bias[None],
    )
    place = (reader_slot % n_lon) * n_lat + reader_slot // n_lon
    next_tile = moved.at[place].get(mode="promise_in_bounds")
    return (features, next_tile)


def solution(mesh):
    split = Mesh(mesh.devices.reshape(4, 2, 2, 2, 4), ("lat_0", "lat_1", "lat_2", "lon_0", "lon_1"))
    return jax.shard_map(
        body,
        mesh=split,
        in_specs=(P(None, LAT, LON), P(LAT + LON, None, None), P(), P(), P(), P(), P()),
        out_specs=(P(None, LAT, LON), P(None, LAT, LON)),
        check_vma=False,
    )
```

```python
import functools

import jax
import jax.numpy as jnp
from jax import lax
from jax.experimental import pallas as pl
from jax.experimental.pallas import tpu as pltpu
from jax.sharding import Mesh
from jax.sharding import PartitionSpec as P

LAT = ("lat_0", "lat_1", "lat_2")
LON = ("lon_0", "lon_1")
LANES = 128
BLOCK = 8
EXTRA = 8
GELU_C = 0.7978845608028654


def gelu(v):
    return (0.5 * v) * (1.0 + jnp.tanh(v * (GELU_C + (GELU_C * 0.044715) * (v * v))))


def conv_kernel(
    channels, rows, cols, hid,
    ends_ref, place_ref, x_ref, top_ref, bottom_ref, left_ref, right_ref, edge_ref,
    w1_raw_ref, b1_ref, w2_raw_ref, b2_ref, moved_ref, out_ref, tile_ref,
    w1_ref, w2_ref, taps_ref, edge_taps_ref, edge_hid_ref, west_ref, mid_ref, east_ref, turned_ref, done_ref, sem,
    held_ref, sums_ref, take_sem,
):
    cells = rows * cols * moved_ref.shape[0]
    first = ends_ref[0] != 0
    last = ends_ref[1] != 0
    lane = lax.broadcasted_iota(jnp.int32, (cols, LANES), 1)
    sub = lax.broadcasted_iota(jnp.int32, (8, LANES), 0)
    sub_hid = lax.broadcasted_iota(jnp.int32, (8, hid), 0)
    over = 2 * channels - LANES

    def weights():
        group = w1_raw_ref.shape[1]
        for a in range(3):
            for b in range(3):
                w1_ref[a * 2 * LANES + b * group : a * 2 * LANES + (b + 1) * group, :] = w1_raw_ref[3 * a + b]
            w1_ref[a * 2 * LANES + 3 * group : (a + 1) * 2 * LANES, :] = jnp.zeros(
                (2 * LANES - 3 * group, hid), jnp.bfloat16
            )
        for tap in range(9):
            w2_ref[tap * hid : (tap + 1) * hid, :] = w2_raw_ref[tap].T

    def norm(raw):
        return (raw.astype(jnp.float32) - mean) * scale

    def pack(minus, zero, plus, lanes):
        turned = pltpu.roll(zero, channels, axis=1)
        low = jnp.where(lanes < channels, minus, turned)
        high = jnp.where(lanes < over, turned, pltpu.roll(plus, over, axis=1))
        return low, high

    def shifted(main, before, after, sub8):
        minus = pltpu.roll(main, 1, axis=0)
        minus = jnp.concatenate([jnp.where(sub8 == 0, before, minus[:8]), minus[8:]], axis=0)
        plus = pltpu.roll(main, cols - 1, axis=0)
        plus = jnp.concatenate([plus[: cols - 8], jnp.where(sub8 == 7, after, plus[cols - 8 :])], axis=0)
        return minus, plus

    def build(row):
        if row < 2:
            raw, keep = top_ref[row], jnp.logical_not(first)
        elif row >= rows + 2:
            raw, keep = bottom_ref[row - rows - 2], jnp.logical_not(last)
        else:
            raw, keep = x_ref[row - 2], None
        main = norm(raw)
        left = norm(left_ref[row])
        right = norm(right_ref[row])
        if keep is not None:
            main = jnp.where(keep, main, 0.0)
            left = jnp.where(keep, left, 0.0)
            right = jnp.where(keep, right, 0.0)
        minus, plus = shifted(main, left[1:2], right[0:1], sub)
        low, high = pack(minus, main, plus, lane)
        taps_ref[row, :, 0:LANES] = low.astype(jnp.bfloat16)
        taps_ref[row, :, LANES : 2 * LANES] = high.astype(jnp.bfloat16)

    def edges():
        tall = edge_ref.shape[2]
        edge_row = lax.broadcasted_iota(jnp.int32, (tall, LANES), 0)
        edge_lane = lax.broadcasted_iota(jnp.int32, (tall, LANES), 1)
        outside = jnp.logical_or(
            jnp.logical_and(first, edge_row < 2), jnp.logical_and(last, edge_row >= rows + 2)
        )
        hid_row = lax.broadcasted_iota(jnp.int32, (tall - 8, hid), 0)
        hid_outside = jnp.logical_or(
            jnp.logical_and(first, hid_row < 1), jnp.logical_and(last, hid_row >= rows + 1)
        )
        for side in range(2):
            parts = [jnp.where(outside, 0.0, norm(edge_ref[side, b])) for b in range(3)]
            low, high = pack(*parts, edge_lane)
            edge_taps_ref[side, :, 0:LANES] = low
            edge_taps_ref[side, :, LANES : 2 * LANES] = high
            stacked = jnp.concatenate(
                [edge_taps_ref[side, a : a + tall - 8, :].astype(jnp.bfloat16) for a in range(3)], axis=1
            )
            value = jnp.dot(stacked, w1_ref[...], preferred_element_type=jnp.float32) + b1_ref[...]
            edge_hid_ref[side] = jnp.where(hid_outside, 0.0, gelu(value))

    def hidden(row, count):
        stacked = jnp.concatenate(
            [taps_ref[row + a : row + a + count].reshape(count * cols, 2 * LANES) for a in range(3)], axis=1
        )
        value = jnp.dot(stacked, w1_ref[...], preferred_element_type=jnp.float32)
        for i in range(count):
            r = row + i
            one = gelu(value[i * cols : (i + 1) * cols] + b1_ref[...])
            if r == 0:
                one = jnp.where(first, 0.0, one)
            elif r == rows + 1:
                one = jnp.where(last, 0.0, one)
            west, east = shifted(one, edge_hid_ref[0, r : r + 1, :], edge_hid_ref[1, r : r + 1, :], sub_hid)
            west_ref[r] = west.astype(jnp.bfloat16)
            mid_ref[r] = one.astype(jnp.bfloat16)
            east_ref[r] = east.astype(jnp.bfloat16)

    def put(t):
        return pltpu.make_async_copy(
            done_ref.at[t], out_ref.at[:, t * BLOCK : (t + 1) * BLOCK, :], sem.at[t]
        )

    def features(t):
        base = t * BLOCK
        stacked = jnp.concatenate(
            [
                ref[base + a : base + a + BLOCK].reshape(BLOCK * cols, hid)
                for a in range(3)
                for ref in (west_ref, mid_ref, east_ref)
            ],
            axis=1,
        )
        value = jnp.dot(stacked, w2_ref[...], preferred_element_type=jnp.float32) + b2_ref[...]
        for i in range(BLOCK):
            turned_ref[t % 2, pl.ds(i, hid, stride=BLOCK), :] = value[i * cols : (i + 1) * cols].T
        done_ref[t] = turned_ref[t % 2].reshape(hid, BLOCK, cols).astype(jnp.bfloat16)
        put(t).start()

    steps = rows // BLOCK
    taken = held_ref.shape[0]
    load_sums = pltpu.make_async_copy(moved_ref.at[:, rows : rows + EXTRA, :], sums_ref, take_sem.at[2])
    load_sums.start()

    @pl.loop(0, taken)
    def _(c):
        pltpu.make_async_copy(moved_ref.at[place_ref[c], 0:rows, :], held_ref.at[c], take_sem.at[0]).start()

    weights()
    load_sums.wait()
    sums = jnp.sum(sums_ref[...].astype(jnp.float32), axis=0)
    mean = (sums[0:1] + sums[1:2] + sums[2:3]) / cells
    square = (sums[3:4] + sums[4:5] + sums[5:6]) / cells
    scale = 1.0 / jnp.sqrt(square - mean * mean + 1e-05)
    scale = jnp.where(lax.broadcasted_iota(jnp.int32, (1, LANES), 1) < channels, scale, 0.0)
    for r in range(BLOCK + 4):
        build(r)
    edges()
    hidden(0, BLOCK + 2)
    for r in range(BLOCK + 4, 2 * BLOCK + 4):
        build(r)
    for t in range(steps):
        if t + 2 < steps:
            for r in range((t + 2) * BLOCK + 4, (t + 3) * BLOCK + 4):
                build(r)
        if t + 1 < steps:
            hidden((t + 1) * BLOCK + 2, BLOCK)
        features(t)
        if t == 1:
            pltpu.make_async_copy(moved_ref.at[0:taken, 0:rows, :], held_ref, take_sem.at[0]).wait()
            pltpu.make_async_copy(held_ref, tile_ref, take_sem.at[1]).start()
    pltpu.make_async_copy(held_ref, tile_ref, take_sem.at[1]).wait()
    for t in range(steps):
        put(t).wait()


def convs(ends, place, x, top, bottom, left, right, edge, w1, b1, w2, b2, moved):
    rows, cols = x.shape[0], x.shape[1]
    hid = w2.shape[1]
    channels = w1.shape[1]
    taken = place.shape[0]
    tall = edge.shape[2]
    vmem = pl.BlockSpec(memory_space=pltpu.VMEM)
    smem = pl.BlockSpec(memory_space=pltpu.SMEM)
    flops = 2 * hid * (rows * cols * 9 * hid + (rows + 2) * (cols + 2) * 3 * 256)
    return pl.pallas_call(
        functools.partial(conv_kernel, channels, rows, cols, hid),
        out_shape=(
            jax.ShapeDtypeStruct((hid, rows, cols), jnp.bfloat16),
            jax.ShapeDtypeStruct((taken, rows, cols), jnp.bfloat16),
        ),
        in_specs=[smem, smem] + [vmem] * 10 + [pl.BlockSpec(memory_space=pl.ANY)],
        out_specs=(pl.BlockSpec(memory_space=pl.ANY),) * 2,
        scratch_shapes=[
            pltpu.VMEM((6 * LANES, hid), jnp.bfloat16),
            pltpu.VMEM((9 * hid, hid), jnp.bfloat16),
            pltpu.VMEM((rows + 4, cols, 2 * LANES), jnp.bfloat16),
            pltpu.VMEM((2, tall, 2 * LANES), jnp.float32),
            pltpu.VMEM((2, tall - 8, hid), jnp.float32),
            pltpu.VMEM((rows + 2, cols, hid), jnp.bfloat16),
            pltpu.VMEM((rows + 2, cols, hid), jnp.bfloat16),
            pltpu.VMEM((rows + 2, cols, hid), jnp.bfloat16),
            pltpu.VMEM((2, hid * BLOCK, cols), jnp.float32),
            pltpu.VMEM((rows // BLOCK, hid, BLOCK, cols), jnp.bfloat16),
            pltpu.SemaphoreType.DMA((rows // BLOCK,)),
            pltpu.VMEM((taken, rows, cols), jnp.bfloat16),
            pltpu.VMEM((moved.shape[0], EXTRA, cols), jnp.bfloat16),
            pltpu.SemaphoreType.DMA((3,)),
        ],
        compiler_params=pltpu.CompilerParams(vmem_limit_bytes=48 * 2**20),
        cost_estimate=pl.CostEstimate(flops=flops, bytes_accessed=8 * 2**20, transcendentals=0),
        name="convs",
    )(ends, place, x, top, bottom, left, right, edge, w1, b1, w2, b2, moved)


def prepare_kernel(
    channels, odd_ref, x_ref, fields_ref,
    turned_ref, one_ref, two_ref, west_ref, east_ref, blocks_ref,
    raw_ref, wide_ref, held_ref, sums_ref, x_sem, in_sem, out_sem, sums_sem,
):
    rows, cols = turned_ref.shape[0], turned_ref.shape[1]
    count = held_ref.shape[0]

    def get(j):
        return pltpu.make_async_copy(fields_ref.at[0, :, j * cols : (j + 1) * cols], held_ref.at[j], in_sem.at[j])

    def put(j):
        return pltpu.make_async_copy(
            held_ref.at[j].reshape(held_ref.shape[1] // rows, rows, cols), blocks_ref.at[j, :, 0:rows, :], out_sem.at[j]
        )

    def put_sums(j):
        return pltpu.make_async_copy(sums_ref, blocks_ref.at[j, :, rows : rows + EXTRA, :], sums_sem.at[j])

    load = pltpu.make_async_copy(x_ref, raw_ref, x_sem)
    load.start()
    for j in range(count):
        get(j).start()
    padded = wide_ref.shape[0] // rows
    wide_ref[channels * rows :, :] = jnp.zeros(((padded - channels) * rows, cols), jnp.float32)
    rest = jnp.zeros((LANES - padded, cols), jnp.float32)
    total = jnp.zeros((padded, cols), jnp.float32)
    square = jnp.zeros((padded, cols), jnp.float32)
    load.wait()
    wide_ref[0 : channels * rows, :] = raw_ref[...].astype(jnp.float32).reshape(channels * rows, cols)
    for r in range(rows):
        one = wide_ref[pl.ds(r, padded, stride=rows), :]
        total += one
        square += one * one
        turned = jnp.concatenate([one, rest], axis=0).T.astype(jnp.bfloat16)
        turned_ref[r] = turned
        west_ref[r] = turned[:2]
        east_ref[r] = turned[cols - 2 :]
        if r % 4 == 3:
            get(r // 4).wait()
            put(r // 4).start()
    odd = odd_ref[0] != 0
    low = turned_ref[0:2]
    high = turned_ref[rows - 2 : rows]
    one_ref[...] = jnp.where(odd, low, high)
    two_ref[...] = jnp.where(odd, high, low)

    def parts(value):
        value = jnp.sum(jnp.concatenate([value, rest], axis=0).T, axis=0, keepdims=True)
        high = value.astype(jnp.bfloat16)
        value = value - high.astype(jnp.float32)
        middle = value.astype(jnp.bfloat16)
        value = value - middle.astype(jnp.float32)
        return [high.astype(jnp.float32), middle.astype(jnp.float32), value]

    both = parts(total) + parts(square) + [jnp.zeros((EXTRA - 6, cols), jnp.float32)]
    both = jnp.concatenate(both, axis=0).astype(jnp.bfloat16)
    sums_ref[...] = jnp.broadcast_to(both[None], sums_ref.shape)
    for j in range(count):
        put_sums(j).start()
    for j in range(count):
        put(j).wait()
        put_sums(j).wait()


def prepare(odd, current, next_fields, n_lon):
    channels, rows, cols = current.shape
    vmem = pl.BlockSpec(memory_space=pltpu.VMEM)
    hbm = pl.BlockSpec(memory_space=pl.ANY)
    height = next_fields.shape[1]
    padded = (channels + 7) // 8 * 8
    return pl.pallas_call(
        functools.partial(prepare_kernel, channels),
        out_shape=(
            jax.ShapeDtypeStruct((rows, cols, LANES), jnp.bfloat16),
            jax.ShapeDtypeStruct((2, cols, LANES), jnp.bfloat16),
            jax.ShapeDtypeStruct((2, cols, LANES), jnp.bfloat16),
            jax.ShapeDtypeStruct((rows, 2, LANES), jnp.bfloat16),
            jax.ShapeDtypeStruct((rows, 2, LANES), jnp.bfloat16),
            jax.ShapeDtypeStruct((n_lon, height // rows, rows + EXTRA, cols), jnp.bfloat16),
        ),
        in_specs=[pl.BlockSpec(memory_space=pltpu.SMEM), hbm, hbm],
        out_specs=(vmem,) * 5 + (hbm,),
        scratch_shapes=[
            pltpu.VMEM((channels, rows, cols), jnp.bfloat16),
            pltpu.VMEM((padded * rows, cols), jnp.float32),
            pltpu.VMEM((n_lon, height, cols), jnp.bfloat16),
            pltpu.VMEM((height // rows, EXTRA, cols), jnp.bfloat16),
            pltpu.SemaphoreType.DMA,
            pltpu.SemaphoreType.DMA((n_lon,)),
            pltpu.SemaphoreType.DMA((n_lon,)),
            pltpu.SemaphoreType.DMA((n_lon,)),
        ],
        compiler_params=pltpu.CompilerParams(vmem_limit_bytes=60 * 2**20),
        cost_estimate=pl.CostEstimate(flops=2**24, bytes_accessed=2**22, transcendentals=0),
        name="prepare",
    )(odd, current, next_fields)


def pairs(count, periodic):
    near = [(i, i ^ 1) for i in range(count)]
    far = [(i, i + 1 if i % 2 else i - 1) for i in range(count)]
    if periodic:
        return near, [(a, b % count) for a, b in far]
    return near, [(a, b) for a, b in far if 0 <= b < count]


def body(current, next_fields, reader_slot, first_weight, first_bias, second_weight, second_bias):
    channels, rows, cols = current.shape
    n_lat = lax.axis_size(LAT)
    n_lon = lax.axis_size(LON)
    at_lat = lax.axis_index(LAT)
    odd_lat = at_lat % 2 == 1
    odd_lon = lax.axis_index(LON) % 2 == 1

    turned, one, two, west, east, blocks = prepare(
        odd_lat.astype(jnp.int32)[None], current, next_fields, n_lon
    )
    near, far = pairs(n_lat, False)
    one = lax.ppermute(one, LAT, near)
    two = lax.ppermute(two, LAT, far)
    moved = lax.all_to_all(
        blocks.reshape(n_lon * n_lat, rows + EXTRA, cols), LON + LAT, split_axis=0, concat_axis=0, tiled=True
    )
    top = jnp.where(odd_lat, one, two)
    bottom = jnp.where(odd_lat, two, one)
    first_cols = jnp.concatenate([top[:, :2], west, bottom[:, :2]], axis=0)
    last_cols = jnp.concatenate([top[:, cols - 2 :], east, bottom[:, cols - 2 :]], axis=0)
    near, far = pairs(n_lon, True)
    one = lax.ppermute(jnp.where(odd_lon, first_cols, last_cols), LON, near)
    two = lax.ppermute(jnp.where(odd_lon, last_cols, first_cols), LON, far)
    left = jnp.where(odd_lon, one, two)
    right = jnp.where(odd_lon, two, one)
    edge = jnp.stack([
        jnp.stack([left[:, 0], left[:, 1], first_cols[:, 0]]),
        jnp.stack([last_cols[:, 1], right[:, 0], right[:, 1]]),
    ])
    edge = jnp.pad(edge, ((0, 0), (0, 0), (0, 48 - rows - 4), (0, 0)))

    w1 = jnp.pad(first_weight.transpose(0, 2, 1), ((0, 0), (0, -channels % 8), (0, 0)))
    ends = jnp.stack([at_lat == 0, at_lat == n_lat - 1]).astype(jnp.int32)
    place = (reader_slot % n_lon) * n_lat + reader_slot // n_lon
    return convs(
        ends, place, turned, top, bottom, left, right, edge,
        w1, first_bias[None], second_weight, second_bias[None], moved,
    )


def solution(mesh):
    split = Mesh(mesh.devices.reshape(4, 2, 2, 2, 4), ("lat_0", "lat_1", "lat_2", "lon_0", "lon_1"))
    return jax.shard_map(
        body,
        mesh=split,
        in_specs=(P(None, LAT, LON), P(LAT + LON, None, None), P(), P(), P(), P(), P()),
        out_specs=(P(None, LAT, LON), P(None, LAT, LON)),
        check_vma=False,
    )
```

```python
import functools

import jax
import jax.numpy as jnp
from jax import lax
from jax.experimental import pallas as pl
from jax.experimental.pallas import tpu as pltpu
from jax.sharding import Mesh
from jax.sharding import PartitionSpec as P

LAT = ("lat_0", "lat_1", "lat_2")
LON = ("lon_0", "lon_1")
LANES = 128
BLOCK = 8
EXTRA = 8
X_PART = 24
SPILL = 13
LAT_COUNT = 16
PREPARE_VMEM = 60 * 2**20
GELU_C = 0.7978845608028654


def gelu(v):
    return (0.5 * v) * (1.0 + jnp.tanh(v * (GELU_C + (GELU_C * 0.044715) * (v * v))))


def conv_kernel(
    channels, rows, cols, hid,
    at_ref, place_ref, x_ref, lat_one_ref, lat_two_ref, sent_one_ref, sent_two_ref, lon_one_ref, lon_two_ref,
    w1_raw_ref, b1_ref, w2_raw_ref, b2_ref, moved_ref, out_ref, tile_ref,
    w1_ref, w2_ref, taps_ref, edge_ref, edge_taps_ref, edge_hid_ref, west_ref, mid_ref, east_ref,
    turned_ref, done_ref, sem, take_sem,
):
    n_lat, n_lon = LAT_COUNT, moved_ref.shape[0] // LAT_COUNT
    cells = rows * cols * moved_ref.shape[0]
    lat, lon = at_ref[0], at_ref[1]
    first = lat == 0
    last = lat == n_lat - 1
    odd_lat = lat % 2 == 1
    odd_lon = lon % 2 == 1
    lane = lax.broadcasted_iota(jnp.int32, (cols, LANES), 1)
    sub = lax.broadcasted_iota(jnp.int32, (8, LANES), 0)
    sub_hid = lax.broadcasted_iota(jnp.int32, (8, hid), 0)
    group = w1_raw_ref.shape[1]
    over = 2 * group - LANES

    def weights():
        for a in range(3):
            for b in range(3):
                w1_ref[a * 2 * LANES + b * group : a * 2 * LANES + (b + 1) * group, :] = w1_raw_ref[3 * a + b]
            w1_ref[a * 2 * LANES + 3 * group : (a + 1) * 2 * LANES, :] = jnp.zeros(
                (2 * LANES - 3 * group, hid), jnp.bfloat16
            )
        for tap in range(9):
            w2_ref[tap * hid : (tap + 1) * hid, :] = w2_raw_ref[tap].T

    def norm(raw):
        return (raw.astype(jnp.float32) - mean) * scale

    def pack(minus, zero, plus, lanes):
        turned = pltpu.roll(zero, group, axis=1)
        low = jnp.where(lanes < group, minus, turned)
        high = jnp.where(lanes < over, turned, pltpu.roll(plus, over, axis=1))
        return low, high

    def shifted(main, before, after, sub8):
        minus = pltpu.roll(main, 1, axis=0)
        minus = jnp.concatenate([jnp.where(sub8 == 0, before, minus[:8]), minus[8:]], axis=0)
        plus = pltpu.roll(main, cols - 1, axis=0)
        plus = jnp.concatenate([plus[: cols - 8], jnp.where(sub8 == 7, after, plus[cols - 8 :])], axis=0)
        return minus, plus

    def lat_row(row):
        if row < 2:
            return jnp.where(odd_lat, lat_one_ref[row], lat_two_ref[row]), jnp.logical_not(first)
        if row >= rows + 2:
            row = row - rows - 2
            return jnp.where(odd_lat, lat_two_ref[row], lat_one_ref[row]), jnp.logical_not(last)
        return x_ref[row - 2], None

    def build(row):
        raw, keep = lat_row(row)
        main = norm(raw)
        if keep is not None:
            main = jnp.where(keep, main, 0.0)
        minus, plus = shifted(main, edge_ref[0, 1, row : row + 1, :], edge_ref[1, 1, row : row + 1, :], sub)
        low, high = pack(minus, main, plus, lane)
        taps_ref[row, :, 0:LANES] = low.astype(jnp.bfloat16)
        taps_ref[row, :, LANES : 2 * LANES] = high.astype(jnp.bfloat16)

    def corner(down, right):
        there = ((lon + right) % n_lon) * n_lat + (lat + down) % n_lat
        block = moved_ref[there, rows : rows + EXTRA, :].astype(jnp.float32)
        line = lax.broadcasted_iota(jnp.int32, (1, LANES), 1)
        split = LANES - channels
        cells = []
        for j in range(2):
            cells.append(block[6 + j : 7 + j])
        for j in range(2):
            head = pltpu.roll(block[6 + j : 7 + j], LANES - channels, axis=1)
            tail = pltpu.roll(block[j : j + 1], LANES - SPILL, axis=1)
            cells.append(jnp.where(line < split, head, tail))
        return cells

    def edges():
        sides = (
            (odd_lon, lon_one_ref, lon_two_ref, sent_one_ref, sent_two_ref),
            (odd_lon, lon_two_ref, lon_one_ref, sent_two_ref, sent_one_ref),
        )
        keep_top = jnp.logical_not(first)
        keep_bottom = jnp.logical_not(last)
        for side, (odd, one_ref, two_ref, own_one_ref, own_two_ref) in enumerate(sides):
            own_part = 2 if side == 0 else 0
            own = jnp.where(odd, own_one_ref[side], own_two_ref[side])
            edge_ref[side, own_part, 2 : rows + 2, :] = norm(own)
            for row in (0, 1, rows + 2, rows + 3):
                raw, keep = lat_row(row)
                value = norm(raw[0:16] if side == 0 else raw[cols - 16 : cols])
                value = value[0:1] if side == 0 else value[15:16]
                edge_ref[side, own_part, row : row + 1, :] = jnp.where(keep, value, 0.0)
            right = 1 if side == 1 else -1
            top = corner(-1, right)
            bottom = corner(1, right)
            for j in range(2):
                part = j + side
                edge_ref[side, part, 2 : rows + 2, :] = norm(jnp.where(odd, one_ref[j], two_ref[j]))
                for i in range(2):
                    edge_ref[side, part, i : i + 1, :] = jnp.where(keep_top, norm(top[2 * i + j]), 0.0)
                    edge_ref[side, part, rows + 2 + i : rows + 3 + i, :] = jnp.where(
                        keep_bottom, norm(bottom[2 * i + j]), 0.0
                    )
        tall = edge_ref.shape[2]
        for side in range(2):
            for part in range(3):
                edge_ref[side, part, rows + 4 : tall, :] = jnp.zeros((tall - rows - 4, LANES), jnp.float32)
        edge_lane = lax.broadcasted_iota(jnp.int32, (tall, LANES), 1)
        hid_row = lax.broadcasted_iota(jnp.int32, (tall - 8, hid), 0)
        hid_outside = jnp.logical_or(
            jnp.logical_and(first, hid_row < 1), jnp.logical_and(last, hid_row >= rows + 1)
        )
        for side in range(2):
            low, high = pack(edge_ref[side, 0], edge_ref[side, 1], edge_ref[side, 2], edge_lane)
            edge_taps_ref[side, :, 0:LANES] = low
            edge_taps_ref[side, :, LANES : 2 * LANES] = high
            stacked = jnp.concatenate(
                [edge_taps_ref[side, a : a + tall - 8, :].astype(jnp.bfloat16) for a in range(3)], axis=1
            )
            value = jnp.dot(stacked, w1_ref[...], preferred_element_type=jnp.float32) + b1_ref[...]
            edge_hid_ref[side] = jnp.where(hid_outside, 0.0, gelu(value))

    def hidden(row, count):
        stacked = jnp.concatenate(
            [taps_ref[row + a : row + a + count].reshape(count * cols, 2 * LANES) for a in range(3)], axis=1
        )
        value = jnp.dot(stacked, w1_ref[...], preferred_element_type=jnp.float32)
        for i in range(count):
            r = row + i
            one = gelu(value[i * cols : (i + 1) * cols] + b1_ref[...])
            if r == 0:
                one = jnp.where(first, 0.0, one)
            elif r == rows + 1:
                one = jnp.where(last, 0.0, one)
            west, east = shifted(one, edge_hid_ref[0, r : r + 1, :], edge_hid_ref[1, r : r + 1, :], sub_hid)
            west_ref[r] = west.astype(jnp.bfloat16)
            mid_ref[r] = one.astype(jnp.bfloat16)
            east_ref[r] = east.astype(jnp.bfloat16)

    def put(t):
        return pltpu.make_async_copy(
            done_ref.at[t], out_ref.at[:, t * BLOCK : (t + 1) * BLOCK, :], sem.at[t]
        )

    def features(t):
        base = t * BLOCK
        stacked = jnp.concatenate(
            [
                ref[base + a : base + a + BLOCK].reshape(BLOCK * cols, hid)
                for a in range(3)
                for ref in (west_ref, mid_ref, east_ref)
            ],
            axis=1,
        )
        value = jnp.dot(stacked, w2_ref[...], preferred_element_type=jnp.float32) + b2_ref[...]
        for i in range(BLOCK):
            turned_ref[t % 2, pl.ds(i, hid, stride=BLOCK), :] = value[i * cols : (i + 1) * cols].T
        done_ref[t] = turned_ref[t % 2].reshape(hid, BLOCK, cols).astype(jnp.bfloat16)
        put(t).start()

    steps = rows // BLOCK
    taken = tile_ref.shape[0]

    @pl.loop(0, taken)
    def _(c):
        pltpu.make_async_copy(moved_ref.at[place_ref[c], 0:rows, :], tile_ref.at[c], take_sem).start()

    weights()
    sums = jnp.sum(moved_ref[:, rows : rows + EXTRA, :].astype(jnp.float32), axis=0)
    line = lax.broadcasted_iota(jnp.int32, (1, LANES), 1)
    mean = (sums[0:1] + sums[1:2] + sums[2:3]) / cells
    square = (sums[3:4] + sums[4:5] + sums[5:6]) / cells
    mean = jnp.where(line < channels, mean, 0.0)
    square = jnp.where(line < channels, square, 0.0)
    scale = 1.0 / jnp.sqrt(square - mean * mean + 1e-05)
    scale = jnp.where(line < channels, scale, 0.0)
    edges()
    for r in range(BLOCK + 4):
        build(r)
    hidden(0, BLOCK + 2)
    for r in range(BLOCK + 4, 2 * BLOCK + 4):
        build(r)
    for t in range(steps):
        if t + 2 < steps:
            for r in range((t + 2) * BLOCK + 4, (t + 3) * BLOCK + 4):
                build(r)
        if t + 1 < steps:
            hidden((t + 1) * BLOCK + 2, BLOCK)
        features(t)
    pltpu.make_async_copy(moved_ref.at[0:taken, 0:rows, :], tile_ref, take_sem).wait()
    for t in range(steps):
        put(t).wait()


def convs(channels, at, place, x, lat_one, lat_two, sent_one, sent_two, lon_one, lon_two, w1, b1, w2, b2, moved):
    rows, cols = x.shape[0], x.shape[1]
    hid = w2.shape[1]
    taken = place.shape[0]
    tall = (rows + 4 + 7) // 8 * 8 + 8
    vmem = pl.BlockSpec(memory_space=pltpu.VMEM)
    smem = pl.BlockSpec(memory_space=pltpu.SMEM)
    hbm = pl.BlockSpec(memory_space=pl.ANY)
    flops = 2 * hid * (rows * cols * 9 * hid + (rows + 2) * (cols + 2) * 3 * 256)
    return pl.pallas_call(
        functools.partial(conv_kernel, channels, rows, cols, hid),
        out_shape=(
            jax.ShapeDtypeStruct((hid, rows, cols), jnp.bfloat16),
            jax.ShapeDtypeStruct((taken, rows, cols), jnp.bfloat16),
        ),
        in_specs=[smem, smem] + [vmem] * 12,
        out_specs=(hbm, hbm),
        scratch_shapes=[
            pltpu.VMEM((6 * LANES, hid), jnp.bfloat16),
            pltpu.VMEM((9 * hid, hid), jnp.bfloat16),
            pltpu.VMEM((rows + 4, cols, 2 * LANES), jnp.bfloat16),
            pltpu.VMEM((2, 3, tall, LANES), jnp.float32),
            pltpu.VMEM((2, tall, 2 * LANES), jnp.float32),
            pltpu.VMEM((2, tall - 8, hid), jnp.float32),
            pltpu.VMEM((rows + 2, cols, hid), jnp.bfloat16),
            pltpu.VMEM((rows + 2, cols, hid), jnp.bfloat16),
            pltpu.VMEM((rows + 2, cols, hid), jnp.bfloat16),
            pltpu.VMEM((2, hid * BLOCK, cols), jnp.float32),
            pltpu.VMEM((rows // BLOCK, hid, BLOCK, cols), jnp.bfloat16),
            pltpu.SemaphoreType.DMA((rows // BLOCK,)),
            pltpu.SemaphoreType.DMA,
        ],
        compiler_params=pltpu.CompilerParams(vmem_limit_bytes=40 * 2**20),
        cost_estimate=pl.CostEstimate(flops=flops, bytes_accessed=8 * 2**20, transcendentals=0),
        name="convs",
    )(at, place, x, lat_one, lat_two, sent_one, sent_two, lon_one, lon_two, w1, b1, w2, b2, moved)


def prepare_kernel(
    channels, at_ref, x_ref, fields_ref,
    turned_ref, lat_one_ref, lat_two_ref, lon_one_ref, lon_two_ref, blocks_ref,
    raw_ref, wide_ref, held_ref, extra_ref, first_ref, last_ref, x_sem, in_sem, out_sem, extra_sem,
):
    rows, cols = turned_ref.shape[0], turned_ref.shape[1]
    n_lon, n_lat = blocks_ref.shape[0], blocks_ref.shape[1]
    lat, lon = at_ref[0], at_ref[1]

    def load(j):
        part = pl.ds(j * X_PART, min(X_PART, channels - j * X_PART))
        return pltpu.make_async_copy(x_ref.at[part], raw_ref.at[part], x_sem.at[j])

    def get(j):
        return pltpu.make_async_copy(fields_ref.at[0, :, j * cols : (j + 1) * cols], held_ref.at[j], in_sem.at[j])

    def put(j):
        return pltpu.make_async_copy(
            held_ref.at[j].reshape(n_lat, rows, cols), blocks_ref.at[j, :, 0:rows, :], out_sem.at[j]
        )

    def put_extra(j):
        return pltpu.make_async_copy(extra_ref.at[j], blocks_ref.at[j, :, rows : rows + EXTRA, :], extra_sem.at[j])

    loads = (channels + X_PART - 1) // X_PART
    for j in range(loads):
        load(j).start()
    for j in range(n_lon):
        get(j).start()
    padded = wide_ref.shape[0] // rows
    wide_ref[channels * rows :, :] = jnp.zeros(((padded - channels) * rows, cols), jnp.float32)
    for j in range(loads):
        load(j).wait()
        low, high = j * X_PART, min((j + 1) * X_PART, channels)
        wide_ref[low * rows : high * rows, :] = (
            raw_ref[low:high].astype(jnp.float32).reshape((high - low) * rows, cols)
        )
    rest = jnp.zeros((LANES - padded, cols), jnp.float32)
    total = jnp.zeros((padded, cols), jnp.float32)
    square = jnp.zeros((padded, cols), jnp.float32)
    for r in range(rows):
        one = wide_ref[pl.ds(r, padded, stride=rows), :]
        total += one
        square += one * one
        turned = jnp.concatenate([one, rest], axis=0).T
        turned_ref[r] = turned.astype(jnp.bfloat16)
        for j in range(2):
            first_ref[j, r : r + 1, :] = turned[j : j + 1]
            last_ref[j, r : r + 1, :] = turned[cols - 2 + j : cols - 1 + j]
        if r % 4 == 3:
            get(r // 4).wait()
            put(r // 4).start()

    def parts(value):
        value = jnp.sum(jnp.concatenate([value, rest], axis=0).T, axis=0, keepdims=True)
        high = value.astype(jnp.bfloat16).astype(jnp.float32)
        value = value - high
        middle = value.astype(jnp.bfloat16).astype(jnp.float32)
        return [high, middle, value - middle]

    sums = parts(total) + parts(square)
    line = lax.broadcasted_iota(jnp.int32, (1, LANES), 1)

    def extra(down, right):
        cols_ref = last_ref if right > 0 else first_ref
        row = rows - 2 if down > 0 else 0
        near = [cols_ref[j, row : row + 1, :] for j in range(2)]
        far = [cols_ref[j, row + 1 : row + 2, :] for j in range(2)]
        spill = [
            jnp.where(
                jnp.logical_and(line >= SPILL + LANES - channels, line < SPILL + channels),
                pltpu.roll(far[j], SPILL, axis=1), sums[j],
            )
            for j in range(2)
        ]
        both = [jnp.where(line < channels, near[j], pltpu.roll(far[j], channels, axis=1)) for j in range(2)]
        return jnp.concatenate(spill + sums[2:] + both, axis=0).astype(jnp.bfloat16)

    extra_ref[...] = jnp.broadcast_to(extra(1, 1)[None, None], extra_ref.shape)
    for down, right in ((1, -1), (-1, 1), (-1, -1)):
        extra_ref[(lon + n_lon + right) % n_lon, (lat + n_lat + down) % n_lat] = extra(down, right)
    for j in range(n_lon):
        put_extra(j).start()
    odd_lat = lat % 2 == 1
    odd_lon = lon % 2 == 1
    low = turned_ref[0:2]
    high = turned_ref[rows - 2 : rows]
    lat_one_ref[...] = jnp.where(odd_lat, low, high)
    lat_two_ref[...] = jnp.where(odd_lat, high, low)
    low = first_ref[...].astype(jnp.bfloat16)
    high = last_ref[...].astype(jnp.bfloat16)
    lon_one_ref[...] = jnp.where(odd_lon, low, high)
    lon_two_ref[...] = jnp.where(odd_lon, high, low)
    for j in range(n_lon):
        put(j).wait()
        put_extra(j).wait()


def prepare(at, current, next_fields, n_lon):
    channels, rows, cols = current.shape
    vmem = pl.BlockSpec(memory_space=pltpu.VMEM)
    hbm = pl.BlockSpec(memory_space=pl.ANY)
    height = next_fields.shape[1]
    padded = (channels + 7) // 8 * 8
    lat_row = jax.ShapeDtypeStruct((2, cols, LANES), jnp.bfloat16)
    lon_row = jax.ShapeDtypeStruct((2, rows, LANES), jnp.bfloat16)
    return pl.pallas_call(
        functools.partial(prepare_kernel, channels),
        out_shape=(
            jax.ShapeDtypeStruct((rows, cols, LANES), jnp.bfloat16),
            lat_row, lat_row, lon_row, lon_row,
            jax.ShapeDtypeStruct((n_lon, height // rows, rows + EXTRA, cols), jnp.bfloat16),
        ),
        in_specs=[pl.BlockSpec(memory_space=pltpu.SMEM), hbm, hbm],
        out_specs=(vmem,) * 5 + (hbm,),
        scratch_shapes=[
            pltpu.VMEM((channels, rows, cols), jnp.bfloat16),
            pltpu.VMEM((padded * rows, cols), jnp.float32),
            pltpu.VMEM((n_lon, height, cols), jnp.bfloat16),
            pltpu.VMEM((n_lon, height // rows, EXTRA, cols), jnp.bfloat16),
            pltpu.VMEM((2, rows, LANES), jnp.float32),
            pltpu.VMEM((2, rows, LANES), jnp.float32),
            pltpu.SemaphoreType.DMA(((channels + X_PART - 1) // X_PART,)),
            pltpu.SemaphoreType.DMA((n_lon,)),
            pltpu.SemaphoreType.DMA((n_lon,)),
            pltpu.SemaphoreType.DMA((n_lon,)),
        ],
        compiler_params=pltpu.CompilerParams(vmem_limit_bytes=PREPARE_VMEM),
        cost_estimate=pl.CostEstimate(flops=2**24, bytes_accessed=2**22, transcendentals=0),
        name="prepare",
    )(at, current, next_fields)


def pairs(count, periodic):
    near = [(i, i ^ 1) for i in range(count)]
    far = [(i, i + 1 if i % 2 else i - 1) for i in range(count)]
    if periodic:
        return near, [(a, b % count) for a, b in far]
    return near, [(a, b) for a, b in far if 0 <= b < count]


def body(current, next_fields, reader_slot, first_weight, first_bias, second_weight, second_bias):
    channels, rows, cols = current.shape
    n_lat = lax.axis_size(LAT)
    n_lon = lax.axis_size(LON)
    at = jnp.stack([lax.axis_index(LAT), lax.axis_index(LON)]).astype(jnp.int32)
    turned, lat_one, lat_two, sent_one, sent_two, blocks = prepare(at, current, next_fields, n_lon)
    moved = lax.all_to_all(
        blocks.reshape(n_lon * n_lat, rows + EXTRA, cols), LON + LAT, split_axis=0, concat_axis=0, tiled=True
    )
    near, far = pairs(n_lat, False)
    lat_one = lax.ppermute(lat_one, LAT, near)
    lat_two = lax.ppermute(lat_two, LAT, far)
    near, far = pairs(n_lon, True)
    lon_one = lax.ppermute(sent_one, LON, near)
    lon_two = lax.ppermute(sent_two, LON, far)
    w1 = jnp.pad(first_weight.transpose(0, 2, 1), ((0, 0), (0, -channels % 8), (0, 0)))
    place = (reader_slot % n_lon) * n_lat + reader_slot // n_lon
    return convs(
        channels, at, place, turned, lat_one, lat_two, sent_one, sent_two, lon_one, lon_two,
        w1, first_bias[None], second_weight, second_bias[None], moved,
    )


def solution(mesh):
    split = Mesh(mesh.devices.reshape(4, 2, 2, 2, 4), ("lat_0", "lat_1", "lat_2", "lon_0", "lon_1"))
    return jax.shard_map(
        body,
        mesh=split,
        in_specs=(P(None, LAT, LON), P(LAT + LON, None, None), P(), P(), P(), P(), P()),
        out_specs=(P(None, LAT, LON), P(None, LAT, LON)),
        check_vma=False,
    )
```

```python
import functools

import jax
import jax.numpy as jnp
from jax import lax
from jax.experimental import pallas as pl
from jax.experimental.pallas import tpu as pltpu
from jax.sharding import Mesh
from jax.sharding import PartitionSpec as P

LAT = ("lat_0", "lat_1", "lat_2")
LON = ("lon_0", "lon_1")
LANES = 128
BLOCK = 8
EXTRA = 8
X_PART = 24
SPILL = 13
GROUP = 72
PREPARE_VMEM = 60 * 2**20
CONVS_VMEM = 40 * 2**20
GELU_C = 0.7978845608028654


def gelu(v):
    return (0.5 * v) * (1.0 + jnp.tanh(v * (GELU_C + (GELU_C * 0.044715) * (v * v))))


def pack(minus, zero, plus, lanes):
    over = 2 * GROUP - LANES
    turned = pltpu.roll(zero, GROUP, axis=1)
    low = jnp.where(lanes < GROUP, minus, turned)
    high = jnp.where(lanes < over, turned, pltpu.roll(plus, over, axis=1))
    return low, high


def shifted(main, before, after, sub8):
    cols = main.shape[0]
    minus = pltpu.roll(main, 1, axis=0)
    minus = jnp.concatenate([jnp.where(sub8 == 0, before, minus[:8]), minus[8:]], axis=0)
    plus = pltpu.roll(main, cols - 1, axis=0)
    plus = jnp.concatenate([plus[: cols - 8], jnp.where(sub8 == 7, after, plus[cols - 8 :])], axis=0)
    return minus, plus


def conv_kernel(
    channels, rows, cols, hid,
    place_ref, taps_hbm_ref, lat_one_ref, lat_two_ref, sent_one_ref, sent_two_ref, lon_one_ref, lon_two_ref,
    w1_hbm_ref, b1_ref, w2_hbm_ref, b2_ref, moved_ref, out_ref, tile_ref,
    raw_taps_ref, w1_ref, w2_ref, taps_ref, edge_ref, edge_taps_ref, edge_hid_ref, west_ref, mid_ref, east_ref,
    turned_ref, done_ref, sem, take_sem, load_sem,
):
    n_lat, n_lon = lax.axis_size(LAT), lax.axis_size(LON)
    cells = rows * cols * moved_ref.shape[0]
    lat, lon = lax.axis_index(LAT), lax.axis_index(LON)
    first = lat == 0
    last = lat == n_lat - 1
    odd_lat = lat % 2 == 1
    odd_lon = lon % 2 == 1
    lane = lax.broadcasted_iota(jnp.int32, (cols, LANES), 1)
    sub = lax.broadcasted_iota(jnp.int32, (8, LANES), 0)
    lane8 = lax.broadcasted_iota(jnp.int32, (8, LANES), 1)
    sub_hid = lax.broadcasted_iota(jnp.int32, (8, hid), 0)
    group = GROUP
    over = 2 * group - LANES

    def norm(raw):
        return (raw.astype(jnp.float32) - mean) * scale

    def lat_row(row):
        if row < 2:
            return jnp.where(odd_lat, lat_one_ref[row], lat_two_ref[row]), jnp.logical_not(first)
        row = row - rows - 2
        return jnp.where(odd_lat, lat_two_ref[row], lat_one_ref[row]), jnp.logical_not(last)

    def build(row):
        before, after = edge_ref[0, 1, row : row + 1, :], edge_ref[1, 1, row : row + 1, :]
        if 2 <= row < rows + 2:
            raw = raw_taps_ref[row - 2].astype(jnp.float32)
            low = (raw[:, 0:LANES] - mean_low) * scale_low
            high = (raw[:, LANES : 2 * LANES] - mean_high) * scale_high
            head = jnp.where(jnp.logical_and(sub == 0, lane8 < group), before, low[:8])
            tail = jnp.where(
                jnp.logical_and(sub == 7, lane8 >= over), pltpu.roll(after, over, axis=1), high[cols - 8 :]
            )
            low = jnp.concatenate([head, low[8:]], axis=0)
            high = jnp.concatenate([high[: cols - 8], tail], axis=0)
        else:
            raw, keep = lat_row(row)
            main = jnp.where(keep, norm(raw), 0.0)
            minus, plus = shifted(main, before, after, sub)
            low, high = pack(minus, main, plus, lane)
        taps_ref[row, :, 0:LANES] = low.astype(jnp.bfloat16)
        taps_ref[row, :, LANES : 2 * LANES] = high.astype(jnp.bfloat16)

    def corner(down, right):
        there = ((lon + right) % n_lon) * n_lat + (lat + down) % n_lat
        block = moved_ref[there, rows : rows + EXTRA, :].astype(jnp.float32)
        line = lax.broadcasted_iota(jnp.int32, (1, LANES), 1)
        split = LANES - channels
        cells = []
        for j in range(2):
            cells.append(block[6 + j : 7 + j])
        for j in range(2):
            head = pltpu.roll(block[6 + j : 7 + j], LANES - channels, axis=1)
            tail = pltpu.roll(block[j : j + 1], LANES - SPILL, axis=1)
            cells.append(jnp.where(line < split, head, tail))
        return cells

    def edges():
        sides = (
            (odd_lon, lon_one_ref, lon_two_ref, sent_one_ref, sent_two_ref),
            (odd_lon, lon_two_ref, lon_one_ref, sent_two_ref, sent_one_ref),
        )
        keep_top = jnp.logical_not(first)
        keep_bottom = jnp.logical_not(last)
        for side, (odd, one_ref, two_ref, own_one_ref, own_two_ref) in enumerate(sides):
            own_part = 2 if side == 0 else 0
            own = jnp.where(odd, own_one_ref[side], own_two_ref[side])
            edge_ref[side, own_part, 2 : rows + 2, :] = norm(own)
            for row in (0, 1, rows + 2, rows + 3):
                raw, keep = lat_row(row)
                value = norm(raw[0:16] if side == 0 else raw[cols - 16 : cols])
                value = value[0:1] if side == 0 else value[15:16]
                edge_ref[side, own_part, row : row + 1, :] = jnp.where(keep, value, 0.0)
            right = 1 if side == 1 else -1
            top = corner(-1, right)
            bottom = corner(1, right)
            for j in range(2):
                part = j + side
                edge_ref[side, part, 2 : rows + 2, :] = norm(jnp.where(odd, one_ref[j], two_ref[j]))
                for i in range(2):
                    edge_ref[side, part, i : i + 1, :] = jnp.where(keep_top, norm(top[2 * i + j]), 0.0)
                    edge_ref[side, part, rows + 2 + i : rows + 3 + i, :] = jnp.where(
                        keep_bottom, norm(bottom[2 * i + j]), 0.0
                    )
        tall = edge_ref.shape[2]
        for side in range(2):
            for part in range(3):
                edge_ref[side, part, rows + 4 : tall, :] = jnp.zeros((tall - rows - 4, LANES), jnp.float32)
        edge_lane = lax.broadcasted_iota(jnp.int32, (tall, LANES), 1)
        hid_row = lax.broadcasted_iota(jnp.int32, (tall - 8, hid), 0)
        hid_outside = jnp.logical_or(
            jnp.logical_and(first, hid_row < 1), jnp.logical_and(last, hid_row >= rows + 1)
        )
        for side in range(2):
            low, high = pack(edge_ref[side, 0], edge_ref[side, 1], edge_ref[side, 2], edge_lane)
            edge_taps_ref[side, :, 0:LANES] = low
            edge_taps_ref[side, :, LANES : 2 * LANES] = high
            stacked = jnp.concatenate(
                [edge_taps_ref[side, a : a + tall - 8, :].astype(jnp.bfloat16) for a in range(3)], axis=1
            )
            value = jnp.dot(stacked, w1_ref[...], preferred_element_type=jnp.float32) + b1_ref[...]
            edge_hid_ref[side] = jnp.where(hid_outside, 0.0, gelu(value))

    def hidden(row, count):
        stacked = jnp.concatenate(
            [taps_ref[row + a : row + a + count].reshape(count * cols, 2 * LANES) for a in range(3)], axis=1
        )
        value = jnp.dot(stacked, w1_ref[...], preferred_element_type=jnp.float32)
        for i in range(count):
            r = row + i
            one = gelu(value[i * cols : (i + 1) * cols] + b1_ref[...])
            if r == 0:
                one = jnp.where(first, 0.0, one)
            elif r == rows + 1:
                one = jnp.where(last, 0.0, one)
            west, east = shifted(one, edge_hid_ref[0, r : r + 1, :], edge_hid_ref[1, r : r + 1, :], sub_hid)
            west_ref[r] = west.astype(jnp.bfloat16)
            mid_ref[r] = one.astype(jnp.bfloat16)
            east_ref[r] = east.astype(jnp.bfloat16)

    def put(t):
        return pltpu.make_async_copy(
            done_ref.at[t], out_ref.at[:, t * BLOCK : (t + 1) * BLOCK, :], sem.at[t]
        )

    def features(t):
        base = t * BLOCK
        stacked = jnp.concatenate(
            [
                ref[base + a : base + a + BLOCK].reshape(BLOCK * cols, hid)
                for a in range(3)
                for ref in (west_ref, mid_ref, east_ref)
            ],
            axis=1,
        )
        value = jnp.dot(stacked, w2_ref[...], preferred_element_type=jnp.float32) + b2_ref[...]
        for i in range(BLOCK):
            turned_ref[t % 2, pl.ds(i, hid, stride=BLOCK), :] = value[i * cols : (i + 1) * cols].T
        done_ref[t] = turned_ref[t % 2].reshape(hid, BLOCK, cols).astype(jnp.bfloat16)
        put(t).start()

    steps = rows // BLOCK
    taken = tile_ref.shape[0]

    def load_taps(t):
        low = 0 if t == 0 else t * BLOCK + 2
        part = pl.ds(low, min((t + 1) * BLOCK + 2, rows) - low)
        return pltpu.make_async_copy(taps_hbm_ref.at[part], raw_taps_ref.at[part], load_sem.at[t])

    load_weights = pltpu.make_async_copy(w2_hbm_ref, w2_ref, load_sem.at[steps])
    load_first = pltpu.make_async_copy(w1_hbm_ref, w1_ref, load_sem.at[steps + 1])
    load_first.start()
    load_taps(0).start()
    load_weights.start()
    for t in range(1, steps):
        load_taps(t).start()

    @pl.loop(0, taken)
    def _(c):
        pltpu.make_async_copy(moved_ref.at[place_ref[c], 0:rows, :], tile_ref.at[c], take_sem).start()

    sums = jnp.sum(moved_ref[:, rows : rows + EXTRA, :].astype(jnp.float32), axis=0)
    line = lax.broadcasted_iota(jnp.int32, (1, LANES), 1)
    mean = (sums[0:1] + sums[1:2] + sums[2:3]) / cells
    square = (sums[3:4] + sums[4:5] + sums[5:6]) / cells
    mean = jnp.where(line < channels, mean, 0.0)
    square = jnp.where(line < channels, square, 0.0)
    scale = 1.0 / jnp.sqrt(square - mean * mean + 1e-05)
    scale = jnp.where(line < channels, scale, 0.0)
    mean_low, mean_high = pack(mean, mean, mean, line)
    scale_low, scale_high = pack(scale, scale, scale, line)
    load_first.wait()
    edges()
    load_taps(0).wait()
    for r in range(BLOCK + 4):
        build(r)
    hidden(0, BLOCK + 2)
    for t in range(1, steps):
        load_taps(t).wait()
    load_weights.wait()
    for r in range(BLOCK + 4, 2 * BLOCK + 4):
        build(r)
    for t in range(steps):
        if t + 2 < steps:
            for r in range((t + 2) * BLOCK + 4, (t + 3) * BLOCK + 4):
                build(r)
        if t + 1 < steps:
            hidden((t + 1) * BLOCK + 2, BLOCK)
        features(t)
    pltpu.make_async_copy(moved_ref.at[0:taken, 0:rows, :], tile_ref, take_sem).wait()
    for t in range(steps):
        put(t).wait()


def convs(channels, place, taps, lat_one, lat_two, sent_one, sent_two, lon_one, lon_two, w1, b1, w2, b2, moved):
    rows, cols = taps.shape[0], taps.shape[1]
    hid = w2.shape[1]
    taken = place.shape[0]
    tall = (rows + 4 + 7) // 8 * 8 + 8
    vmem = pl.BlockSpec(memory_space=pltpu.VMEM)
    smem = pl.BlockSpec(memory_space=pltpu.SMEM)
    hbm = pl.BlockSpec(memory_space=pl.ANY)
    flops = 2 * hid * (rows * cols * 9 * hid + (rows + 2) * (cols + 2) * 3 * 256)
    return pl.pallas_call(
        functools.partial(conv_kernel, channels, rows, cols, hid),
        out_shape=(
            jax.ShapeDtypeStruct((hid, rows, cols), jnp.bfloat16),
            jax.ShapeDtypeStruct((taken, rows, cols), jnp.bfloat16),
        ),
        in_specs=[smem, hbm] + [vmem] * 6 + [hbm, vmem, hbm, vmem, vmem],
        out_specs=(hbm, hbm),
        scratch_shapes=[
            pltpu.VMEM((rows, cols, 2 * LANES), jnp.bfloat16),
            pltpu.VMEM((6 * LANES, hid), jnp.bfloat16),
            pltpu.VMEM((9 * hid, hid), jnp.bfloat16),
            pltpu.VMEM((rows + 4, cols, 2 * LANES), jnp.bfloat16),
            pltpu.VMEM((2, 3, tall, LANES), jnp.float32),
            pltpu.VMEM((2, tall, 2 * LANES), jnp.float32),
            pltpu.VMEM((2, tall - 8, hid), jnp.float32),
            pltpu.VMEM((rows + 2, cols, hid), jnp.bfloat16),
            pltpu.VMEM((rows + 2, cols, hid), jnp.bfloat16),
            pltpu.VMEM((rows + 2, cols, hid), jnp.bfloat16),
            pltpu.VMEM((2, hid * BLOCK, cols), jnp.float32),
            pltpu.VMEM((rows // BLOCK, hid, BLOCK, cols), jnp.bfloat16),
            pltpu.SemaphoreType.DMA((rows // BLOCK,)),
            pltpu.SemaphoreType.DMA,
            pltpu.SemaphoreType.DMA((rows // BLOCK + 2,)),
        ],
        compiler_params=pltpu.CompilerParams(vmem_limit_bytes=CONVS_VMEM),
        cost_estimate=pl.CostEstimate(flops=flops, bytes_accessed=8 * 2**20, transcendentals=0),
        name="convs",
    )(place, taps, lat_one, lat_two, sent_one, sent_two, lon_one, lon_two, w1, b1, w2, b2, moved)


def stage_kernel(x_ref, w1_raw_ref, w2_raw_ref, taps_ref, w1_ref, w2_ref, wide_ref):
    channels, rows, cols = x_ref.shape
    hid = w2_ref.shape[1]
    padded = wide_ref.shape[0] // rows
    wide_ref[channels * rows :, :] = jnp.zeros(((padded - channels) * rows, cols), jnp.float32)
    wide_ref[0 : channels * rows, :] = x_ref[...].astype(jnp.float32).reshape(channels * rows, cols)
    rest = jnp.zeros((LANES - padded, cols), jnp.float32)
    lane = lax.broadcasted_iota(jnp.int32, (cols, LANES), 1)
    sub = lax.broadcasted_iota(jnp.int32, (8, LANES), 0)
    for r in range(rows):
        one = wide_ref[pl.ds(r, padded, stride=rows), :]
        main = jnp.concatenate([one, rest], axis=0).T
        minus, plus = shifted(main, 0.0, 0.0, sub)
        low, high = pack(minus, main, plus, lane)
        taps_ref[r, :, 0:LANES] = low.astype(jnp.bfloat16)
        taps_ref[r, :, LANES : 2 * LANES] = high.astype(jnp.bfloat16)
    group = w1_raw_ref.shape[1]
    for a in range(3):
        for b in range(3):
            w1_ref[a * 2 * LANES + b * group : a * 2 * LANES + (b + 1) * group, :] = w1_raw_ref[3 * a + b]
        w1_ref[a * 2 * LANES + 3 * group : (a + 1) * 2 * LANES, :] = jnp.zeros(
            (2 * LANES - 3 * group, hid), jnp.bfloat16
        )
    for tap in range(9):
        w2_ref[tap * hid : (tap + 1) * hid, :] = w2_raw_ref[tap].T


def stage(current, w1, w2):
    _, rows, cols = current.shape
    hid = w2.shape[1]
    vmem = pl.BlockSpec(memory_space=pltpu.VMEM)
    return pl.pallas_call(
        stage_kernel,
        out_shape=(
            jax.ShapeDtypeStruct((rows, cols, 2 * LANES), jnp.bfloat16),
            jax.ShapeDtypeStruct((6 * LANES, hid), jnp.bfloat16),
            jax.ShapeDtypeStruct((9 * hid, hid), jnp.bfloat16),
        ),
        in_specs=[vmem] * 3,
        out_specs=(vmem,) * 3,
        scratch_shapes=[pltpu.VMEM((GROUP * rows, cols), jnp.float32)],
        compiler_params=pltpu.CompilerParams(vmem_limit_bytes=16 * 2**20),
        cost_estimate=pl.CostEstimate(flops=2**25, bytes_accessed=2**22, transcendentals=0),
        name="stage",
    )(current, w1, w2)


def prepare_kernel(
    channels, x_ref, fields_ref,
    lat_one_ref, lat_two_ref, lon_one_ref, lon_two_ref, blocks_ref,
    raw_ref, wide_ref, gather_ref, partial_ref, held_ref, extra_ref, lat_ref, lon_ref, first_ref, last_ref,
    x_sem, in_sem, out_sem, extra_sem, halo_sem,
):
    rows, cols = raw_ref.shape[1], raw_ref.shape[2]
    n_lon, n_lat = blocks_ref.shape[0], blocks_ref.shape[1]
    lat, lon = lax.axis_index(LAT), lax.axis_index(LON)

    def load(j):
        part = pl.ds(j * X_PART, min(X_PART, channels - j * X_PART))
        return pltpu.make_async_copy(x_ref.at[part], raw_ref.at[part], x_sem.at[j])

    def get(j):
        return pltpu.make_async_copy(fields_ref.at[0, :, j * cols : (j + 1) * cols], held_ref.at[j], in_sem.at[j])

    def put(j):
        return pltpu.make_async_copy(
            held_ref.at[j].reshape(n_lat, rows, cols), blocks_ref.at[j, :, 0:rows, :], out_sem.at[j]
        )

    def put_extra(j):
        return pltpu.make_async_copy(extra_ref.at[j], blocks_ref.at[j, :, rows : rows + EXTRA, :], extra_sem.at[j])

    halos = [
        pltpu.make_async_copy(lat_ref.at[0], lat_one_ref, halo_sem.at[0]),
        pltpu.make_async_copy(lat_ref.at[1], lat_two_ref, halo_sem.at[1]),
        pltpu.make_async_copy(lon_ref.at[0], lon_one_ref, halo_sem.at[2]),
        pltpu.make_async_copy(lon_ref.at[1], lon_two_ref, halo_sem.at[3]),
    ]
    loads = (channels + X_PART - 1) // X_PART
    for j in range(loads):
        load(j).start()
    for j in range(n_lon):
        get(j).start()
    padded = wide_ref.shape[0] // rows
    wide_ref[channels * rows :, :] = jnp.zeros(((padded - channels) * rows, cols), jnp.float32)
    partial_ref[:, channels * 8 :, :] = jnp.zeros((2, (padded - channels) * 8, cols), jnp.float32)
    for j in range(loads):
        load(j).wait()
        low, high = j * X_PART, min((j + 1) * X_PART, channels)
        count = high - low
        value = raw_ref[low:high].astype(jnp.float32)
        wide_ref[low * rows : high * rows, :] = value.reshape(count * rows, cols)
        value = value.reshape(count, rows // 8, 8, cols)
        partial_ref[0, low * 8 : high * 8, :] = jnp.sum(value, axis=1).reshape(count * 8, cols)
        partial_ref[1, low * 8 : high * 8, :] = jnp.sum(value * value, axis=1).reshape(count * 8, cols)
    rest = jnp.zeros((LANES - padded, cols), jnp.float32)
    odd_lat = lat % 2 == 1
    odd_lon = lon % 2 == 1
    lane = lax.broadcasted_iota(jnp.int32, (padded, cols), 1)
    columns = jnp.zeros((padded, cols), jnp.float32)
    kept = {}
    for r in range(rows):
        one = wide_ref[pl.ds(r, padded, stride=rows), :]
        columns = jnp.where(lane // 4 == r, pltpu.roll(one, (2 + 4 * r) % cols, axis=1), columns)
        if r in (0, 1, rows - 2, rows - 1):
            kept[r] = jnp.concatenate([one, rest], axis=0).T
    for j in range(2):
        low, high = kept[j], kept[rows - 2 + j]
        lat_ref[0, j] = jnp.where(odd_lat, low, high).astype(jnp.bfloat16)
        lat_ref[1, j] = jnp.where(odd_lat, high, low).astype(jnp.bfloat16)
    halos[0].start()
    halos[1].start()
    gather_ref[...] = jnp.concatenate([columns, rest], axis=0).T
    for j in range(2):
        last_ref[j] = gather_ref[pl.ds(j, rows, stride=4), :]
        first_ref[j] = gather_ref[pl.ds(2 + j, rows, stride=4), :]
    low, high = first_ref[...], last_ref[...]
    lon_ref[0] = jnp.where(odd_lon, low, high).astype(jnp.bfloat16)
    lon_ref[1] = jnp.where(odd_lon, high, low).astype(jnp.bfloat16)
    halos[2].start()
    halos[3].start()

    def parts(which):
        value = partial_ref[which, pl.ds(0, padded, stride=8), :]
        for i in range(1, 8):
            value = value + partial_ref[which, pl.ds(i, padded, stride=8), :]
        value = jnp.sum(jnp.concatenate([value, rest], axis=0).T, axis=0, keepdims=True)
        high = value.astype(jnp.bfloat16).astype(jnp.float32)
        value = value - high
        middle = value.astype(jnp.bfloat16).astype(jnp.float32)
        return [high, middle, value - middle]

    sums = parts(0) + parts(1)
    line = lax.broadcasted_iota(jnp.int32, (1, LANES), 1)

    def extra(down, right):
        cols_ref = last_ref if right > 0 else first_ref
        row = rows - 2 if down > 0 else 0
        near = [cols_ref[j, row : row + 1, :] for j in range(2)]
        far = [cols_ref[j, row + 1 : row + 2, :] for j in range(2)]
        spill = [
            jnp.where(
                jnp.logical_and(line >= SPILL + LANES - channels, line < SPILL + channels),
                pltpu.roll(far[j], SPILL, axis=1), sums[j],
            )
            for j in range(2)
        ]
        both = [jnp.where(line < channels, near[j], pltpu.roll(far[j], channels, axis=1)) for j in range(2)]
        return jnp.concatenate(spill + sums[2:] + both, axis=0).astype(jnp.bfloat16)

    extra_ref[...] = jnp.broadcast_to(extra(1, 1)[None, None], extra_ref.shape)
    for down, right in ((1, -1), (-1, 1), (-1, -1)):
        extra_ref[(lon + n_lon + right) % n_lon, (lat + n_lat + down) % n_lat] = extra(down, right)
    for j in range(n_lon):
        put_extra(j).start()
    for j in range(n_lon):
        get(j).wait()
        put(j).start()
    for j in range(n_lon):
        put(j).wait()
        put_extra(j).wait()
    for halo in halos:
        halo.wait()


def prepare(current, next_fields, n_lon):
    channels, rows, cols = current.shape
    hbm = pl.BlockSpec(memory_space=pl.ANY)
    height = next_fields.shape[1]
    lat_row = jax.ShapeDtypeStruct((2, cols, LANES), jnp.bfloat16)
    lon_row = jax.ShapeDtypeStruct((2, rows, LANES), jnp.bfloat16)
    return pl.pallas_call(
        functools.partial(prepare_kernel, channels),
        out_shape=(
            lat_row, lat_row, lon_row, lon_row,
            jax.ShapeDtypeStruct((n_lon, height // rows, rows + EXTRA, cols), jnp.bfloat16),
        ),
        in_specs=[hbm, hbm],
        out_specs=(hbm,) * 5,
        scratch_shapes=[
            pltpu.VMEM((channels, rows, cols), jnp.bfloat16),
            pltpu.VMEM((GROUP * rows, cols), jnp.float32),
            pltpu.VMEM((cols, LANES), jnp.float32),
            pltpu.VMEM((2, GROUP * 8, cols), jnp.float32),
            pltpu.VMEM((n_lon, height, cols), jnp.bfloat16),
            pltpu.VMEM((n_lon, height // rows, EXTRA, cols), jnp.bfloat16),
            pltpu.VMEM((2, 2, cols, LANES), jnp.bfloat16),
            pltpu.VMEM((2, 2, rows, LANES), jnp.bfloat16),
            pltpu.VMEM((2, rows, LANES), jnp.float32),
            pltpu.VMEM((2, rows, LANES), jnp.float32),
            pltpu.SemaphoreType.DMA(((channels + X_PART - 1) // X_PART,)),
            pltpu.SemaphoreType.DMA((n_lon,)),
            pltpu.SemaphoreType.DMA((n_lon,)),
            pltpu.SemaphoreType.DMA((n_lon,)),
            pltpu.SemaphoreType.DMA((4,)),
        ],
        compiler_params=pltpu.CompilerParams(vmem_limit_bytes=PREPARE_VMEM),
        cost_estimate=pl.CostEstimate(flops=2**24, bytes_accessed=2**22, transcendentals=0),
        name="prepare",
    )(current, next_fields)


def in_hbm(array):
    return pltpu.with_memory_space_constraint(array, pltpu.HBM)


def pairs(count, periodic):
    near = [(i, i ^ 1) for i in range(count)]
    far = [(i, i + 1 if i % 2 else i - 1) for i in range(count)]
    if periodic:
        return near, [(a, b % count) for a, b in far]
    return near, [(a, b) for a, b in far if 0 <= b < count]


def body(current, next_fields, reader_slot, first_weight, first_bias, second_weight, second_bias):
    channels, rows, cols = current.shape
    n_lat = lax.axis_size(LAT)
    n_lon = lax.axis_size(LON)
    lat_one, lat_two, sent_one, sent_two, blocks = prepare(current, next_fields, n_lon)
    moved = lax.all_to_all(
        blocks.reshape(n_lon * n_lat, rows + EXTRA, cols), LON + LAT, split_axis=0, concat_axis=0, tiled=True
    )
    near, far = pairs(n_lat, False)
    lat_one = lax.ppermute(lat_one, LAT, near)
    lat_two = lax.ppermute(lat_two, LAT, far)
    near, far = pairs(n_lon, True)
    lon_one = lax.ppermute(sent_one, LON, near)
    lon_two = lax.ppermute(sent_two, LON, far)
    w1 = jnp.pad(first_weight.transpose(0, 2, 1), ((0, 0), (0, GROUP - channels), (0, 0)))
    taps, w1, w2 = stage(current, w1, second_weight)
    place = (reader_slot % n_lon) * n_lat + reader_slot // n_lon
    taps, w1, w2 = in_hbm(taps), in_hbm(w1), in_hbm(w2)
    return convs(
        channels, place, taps, lat_one, lat_two, sent_one, sent_two, lon_one, lon_two,
        w1, first_bias[None], w2, second_bias[None], moved,
    )


def solution(mesh):
    split = Mesh(mesh.devices.reshape(4, 2, 2, 2, 4), ("lat_0", "lat_1", "lat_2", "lon_0", "lon_1"))
    return jax.shard_map(
        body,
        mesh=split,
        in_specs=(P(None, LAT, LON), P(LAT + LON, None, None), P(), P(), P(), P(), P()),
        out_specs=(P(None, LAT, LON), P(None, LAT, LON)),
        check_vma=False,
    )
```

```python
import functools

import jax
import jax.numpy as jnp
from jax import lax
from jax.experimental import pallas as pl
from jax.experimental.pallas import tpu as pltpu
from jax.sharding import Mesh
from jax.sharding import PartitionSpec as P

LAT = ("lat_0", "lat_1", "lat_2")
LON = ("lon_0", "lon_1")
LANES = 128
BLOCK = 8
UNIT = 2
EXTRA = 8
X_PART = 24
SPILL = 13
GROUP = 72
PREPARE_VMEM = 60 * 2**20
CONVS_VMEM = 40 * 2**20
GELU_C = 0.7978845608028654


def gelu(v):
    return (0.5 * v) * (1.0 + jnp.tanh(v * (GELU_C + (GELU_C * 0.044715) * (v * v))))


def pack(minus, zero, plus, lanes):
    over = 2 * GROUP - LANES
    turned = pltpu.roll(zero, GROUP, axis=1)
    low = jnp.where(lanes < GROUP, minus, turned)
    high = jnp.where(lanes < over, turned, pltpu.roll(plus, over, axis=1))
    return low, high


def shifted(main, before, after, sub8):
    cols = main.shape[0]
    minus = pltpu.roll(main, 1, axis=0)
    minus = jnp.concatenate([jnp.where(sub8 == 0, before, minus[:8]), minus[8:]], axis=0)
    plus = pltpu.roll(main, cols - 1, axis=0)
    plus = jnp.concatenate([plus[: cols - 8], jnp.where(sub8 == 7, after, plus[cols - 8 :])], axis=0)
    return minus, plus


def conv_kernel(
    channels, rows, cols, hid,
    place_ref, taps_hbm_ref, lat_one_ref, lat_two_ref, sent_one_ref, sent_two_ref, lon_one_ref, lon_two_ref,
    w1_hbm_ref, b1_ref, w2_hbm_ref, b2_ref, moved_ref, out_ref, tile_ref,
    raw_taps_ref, w1_ref, w2_ref, taps_ref, edge_ref, edge_taps_ref, edge_hid_ref, west_ref, mid_ref, east_ref,
    turned_ref, done_ref, sem, take_sem, load_sem,
):
    n_lat, n_lon = lax.axis_size(LAT), lax.axis_size(LON)
    cells = rows * cols * moved_ref.shape[0]
    lat, lon = lax.axis_index(LAT), lax.axis_index(LON)
    first = lat == 0
    last = lat == n_lat - 1
    odd_lat = lat % 2 == 1
    odd_lon = lon % 2 == 1
    lane = lax.broadcasted_iota(jnp.int32, (cols, LANES), 1)
    sub = lax.broadcasted_iota(jnp.int32, (8, LANES), 0)
    lane8 = lax.broadcasted_iota(jnp.int32, (8, LANES), 1)
    sub_hid = lax.broadcasted_iota(jnp.int32, (8, hid), 0)
    group = GROUP
    over = 2 * group - LANES

    def norm(raw):
        return (raw.astype(jnp.float32) - mean) * scale

    def lat_row(row):
        if row < 2:
            return jnp.where(odd_lat, lat_one_ref[row], lat_two_ref[row]), jnp.logical_not(first)
        row = row - rows - 2
        return jnp.where(odd_lat, lat_two_ref[row], lat_one_ref[row]), jnp.logical_not(last)

    def build(row):
        before, after = edge_ref[0, 1, row : row + 1, :], edge_ref[1, 1, row : row + 1, :]
        if 2 <= row < rows + 2:
            raw = raw_taps_ref[row - 2].astype(jnp.float32)
            low = (raw[:, 0:LANES] - mean_low) * scale_low
            high = (raw[:, LANES : 2 * LANES] - mean_high) * scale_high
            head = jnp.where(jnp.logical_and(sub == 0, lane8 < group), before, low[:8])
            tail = jnp.where(
                jnp.logical_and(sub == 7, lane8 >= over), pltpu.roll(after, over, axis=1), high[cols - 8 :]
            )
            low = jnp.concatenate([head, low[8:]], axis=0)
            high = jnp.concatenate([high[: cols - 8], tail], axis=0)
        else:
            raw, keep = lat_row(row)
            main = jnp.where(keep, norm(raw), 0.0)
            minus, plus = shifted(main, before, after, sub)
            low, high = pack(minus, main, plus, lane)
        taps_ref[row, :, 0:LANES] = low.astype(jnp.bfloat16)
        taps_ref[row, :, LANES : 2 * LANES] = high.astype(jnp.bfloat16)

    def corner(down, right):
        there = ((lon + right) % n_lon) * n_lat + (lat + down) % n_lat
        block = moved_ref[there, rows : rows + EXTRA, :].astype(jnp.float32)
        line = lax.broadcasted_iota(jnp.int32, (1, LANES), 1)
        split = LANES - channels
        cells = []
        for j in range(2):
            cells.append(block[6 + j : 7 + j])
        for j in range(2):
            head = pltpu.roll(block[6 + j : 7 + j], LANES - channels, axis=1)
            tail = pltpu.roll(block[j : j + 1], LANES - SPILL, axis=1)
            cells.append(jnp.where(line < split, head, tail))
        return cells

    def edges():
        sides = (
            (odd_lon, lon_one_ref, lon_two_ref, sent_one_ref, sent_two_ref),
            (odd_lon, lon_two_ref, lon_one_ref, sent_two_ref, sent_one_ref),
        )
        keep_top = jnp.logical_not(first)
        keep_bottom = jnp.logical_not(last)
        for side, (odd, one_ref, two_ref, own_one_ref, own_two_ref) in enumerate(sides):
            own_part = 2 if side == 0 else 0
            own = jnp.where(odd, own_one_ref[side], own_two_ref[side])
            edge_ref[side, own_part, 2 : rows + 2, :] = norm(own)
            for row in (0, 1, rows + 2, rows + 3):
                raw, keep = lat_row(row)
                value = norm(raw[0:16] if side == 0 else raw[cols - 16 : cols])
                value = value[0:1] if side == 0 else value[15:16]
                edge_ref[side, own_part, row : row + 1, :] = jnp.where(keep, value, 0.0)
            right = 1 if side == 1 else -1
            top = corner(-1, right)
            bottom = corner(1, right)
            for j in range(2):
                part = j + side
                edge_ref[side, part, 2 : rows + 2, :] = norm(jnp.where(odd, one_ref[j], two_ref[j]))
                for i in range(2):
                    edge_ref[side, part, i : i + 1, :] = jnp.where(keep_top, norm(top[2 * i + j]), 0.0)
                    edge_ref[side, part, rows + 2 + i : rows + 3 + i, :] = jnp.where(
                        keep_bottom, norm(bottom[2 * i + j]), 0.0
                    )
        tall = edge_ref.shape[2]
        for side in range(2):
            for part in range(3):
                edge_ref[side, part, rows + 4 : tall, :] = jnp.zeros((tall - rows - 4, LANES), jnp.float32)

    def edges_hidden():
        tall = edge_ref.shape[2]
        edge_lane = lax.broadcasted_iota(jnp.int32, (tall, LANES), 1)
        hid_row = lax.broadcasted_iota(jnp.int32, (tall - 8, hid), 0)
        hid_outside = jnp.logical_or(
            jnp.logical_and(first, hid_row < 1), jnp.logical_and(last, hid_row >= rows + 1)
        )
        for side in range(2):
            low, high = pack(edge_ref[side, 0], edge_ref[side, 1], edge_ref[side, 2], edge_lane)
            edge_taps_ref[side, :, 0:LANES] = low
            edge_taps_ref[side, :, LANES : 2 * LANES] = high
            stacked = jnp.concatenate(
                [edge_taps_ref[side, a : a + tall - 8, :].astype(jnp.bfloat16) for a in range(3)], axis=1
            )
            value = jnp.dot(stacked, w1_ref[...], preferred_element_type=jnp.float32) + b1_ref[...]
            edge_hid_ref[side] = jnp.where(hid_outside, 0.0, gelu(value))

    def hidden(row, count):
        stacked = jnp.concatenate(
            [taps_ref[row + a : row + a + count].reshape(count * cols, 2 * LANES) for a in range(3)], axis=1
        )
        value = jnp.dot(stacked, w1_ref[...], preferred_element_type=jnp.float32)
        for i in range(count):
            r = row + i
            one = gelu(value[i * cols : (i + 1) * cols] + b1_ref[...])
            if r == 0:
                one = jnp.where(first, 0.0, one)
            elif r == rows + 1:
                one = jnp.where(last, 0.0, one)
            west, east = shifted(one, edge_hid_ref[0, r : r + 1, :], edge_hid_ref[1, r : r + 1, :], sub_hid)
            west_ref[r] = west.astype(jnp.bfloat16)
            mid_ref[r] = one.astype(jnp.bfloat16)
            east_ref[r] = east.astype(jnp.bfloat16)

    def put(t):
        return pltpu.make_async_copy(
            done_ref.at[t], out_ref.at[:, t * BLOCK : (t + 1) * BLOCK, :], sem.at[t]
        )

    def features(u):
        base = u * UNIT
        stacked = jnp.concatenate(
            [
                ref[base + a : base + a + UNIT].reshape(UNIT * cols, hid)
                for a in range(3)
                for ref in (west_ref, mid_ref, east_ref)
            ],
            axis=1,
        )
        value = jnp.dot(stacked, w2_ref[...], preferred_element_type=jnp.float32) + b2_ref[...]
        t, at = base // BLOCK, base % BLOCK
        for i in range(UNIT):
            turned_ref[t % 2, pl.ds(at + i, hid, stride=BLOCK), :] = value[i * cols : (i + 1) * cols].T
        if at + UNIT == BLOCK:
            done_ref[t] = turned_ref[t % 2].reshape(hid, BLOCK, cols).astype(jnp.bfloat16)
            put(t).start()

    steps = rows // BLOCK
    taken = tile_ref.shape[0]

    def load_taps(t):
        low = 0 if t == 0 else t * BLOCK + 2
        part = pl.ds(low, min((t + 1) * BLOCK + 2, rows) - low)
        return pltpu.make_async_copy(taps_hbm_ref.at[part], raw_taps_ref.at[part], load_sem.at[t])

    load_weights = pltpu.make_async_copy(w2_hbm_ref, w2_ref, load_sem.at[steps])
    load_first = pltpu.make_async_copy(w1_hbm_ref, w1_ref, load_sem.at[steps + 1])
    load_taps(0).start()
    load_first.start()
    load_weights.start()
    for t in range(1, steps):
        load_taps(t).start()

    sums = jnp.sum(moved_ref[:, rows : rows + EXTRA, :].astype(jnp.float32), axis=0)
    line = lax.broadcasted_iota(jnp.int32, (1, LANES), 1)
    mean = (sums[0:1] + sums[1:2] + sums[2:3]) / cells
    square = (sums[3:4] + sums[4:5] + sums[5:6]) / cells
    mean = jnp.where(line < channels, mean, 0.0)
    square = jnp.where(line < channels, square, 0.0)
    scale = 1.0 / jnp.sqrt(square - mean * mean + 1e-05)
    scale = jnp.where(line < channels, scale, 0.0)
    mean_low, mean_high = pack(mean, mean, mean, line)
    scale_low, scale_high = pack(scale, scale, scale, line)
    edges()
    load_taps(0).wait()
    for r in range(UNIT + 4):
        build(r)
    load_first.wait()
    edges_hidden()
    hidden(0, UNIT + 2)
    for c in range(taken):
        pltpu.make_async_copy(moved_ref.at[place_ref[c], 0:rows, :], tile_ref.at[c], take_sem).start()
    for t in range(1, steps):
        load_taps(t).wait()
    load_weights.wait()
    units = rows // UNIT

    def more(u):
        if u < units:
            for r in range(u * UNIT + 4, (u + 1) * UNIT + 4):
                build(r)

    more(1)
    for u in range(units):
        more(u + 2)
        if u + 1 < units:
            hidden((u + 1) * UNIT + 2, UNIT)
        features(u)
    pltpu.make_async_copy(moved_ref.at[0:taken, 0:rows, :], tile_ref, take_sem).wait()
    for t in range(steps):
        put(t).wait()


def convs(channels, place, taps, lat_one, lat_two, sent_one, sent_two, lon_one, lon_two, w1, b1, w2, b2, moved):
    rows, cols = taps.shape[0], taps.shape[1]
    hid = w2.shape[1]
    taken = place.shape[0]
    tall = (rows + 4 + 7) // 8 * 8 + 8
    vmem = pl.BlockSpec(memory_space=pltpu.VMEM)
    smem = pl.BlockSpec(memory_space=pltpu.SMEM)
    hbm = pl.BlockSpec(memory_space=pl.ANY)
    flops = 2 * hid * (rows * cols * 9 * hid + (rows + 2) * (cols + 2) * 3 * 256)
    return pl.pallas_call(
        functools.partial(conv_kernel, channels, rows, cols, hid),
        out_shape=(
            jax.ShapeDtypeStruct((hid, rows, cols), jnp.bfloat16),
            jax.ShapeDtypeStruct((taken, rows, cols), jnp.bfloat16),
        ),
        in_specs=[smem, hbm] + [vmem] * 6 + [hbm, vmem, hbm, vmem, vmem],
        out_specs=(hbm, hbm),
        scratch_shapes=[
            pltpu.VMEM((rows, cols, 2 * LANES), jnp.bfloat16),
            pltpu.VMEM((6 * LANES, hid), jnp.bfloat16),
            pltpu.VMEM((9 * hid, hid), jnp.bfloat16),
            pltpu.VMEM((rows + 4, cols, 2 * LANES), jnp.bfloat16),
            pltpu.VMEM((2, 3, tall, LANES), jnp.float32),
            pltpu.VMEM((2, tall, 2 * LANES), jnp.float32),
            pltpu.VMEM((2, tall - 8, hid), jnp.float32),
            pltpu.VMEM((rows + 2, cols, hid), jnp.bfloat16),
            pltpu.VMEM((rows + 2, cols, hid), jnp.bfloat16),
            pltpu.VMEM((rows + 2, cols, hid), jnp.bfloat16),
            pltpu.VMEM((2, hid * BLOCK, cols), jnp.float32),
            pltpu.VMEM((rows // BLOCK, hid, BLOCK, cols), jnp.bfloat16),
            pltpu.SemaphoreType.DMA((rows // BLOCK,)),
            pltpu.SemaphoreType.DMA,
            pltpu.SemaphoreType.DMA((rows // BLOCK + 2,)),
        ],
        compiler_params=pltpu.CompilerParams(vmem_limit_bytes=CONVS_VMEM),
        cost_estimate=pl.CostEstimate(flops=flops, bytes_accessed=8 * 2**20, transcendentals=0),
        name="convs",
    )(place, taps, lat_one, lat_two, sent_one, sent_two, lon_one, lon_two, w1, b1, w2, b2, moved)


def stage_kernel(x_ref, w1_raw_ref, w2_raw_ref, taps_ref, w1_ref, w2_ref, wide_ref):
    channels, rows, cols = x_ref.shape
    hid = w2_ref.shape[1]
    padded = wide_ref.shape[1] // 8
    value = x_ref[...].astype(jnp.float32)
    for q in range(rows // 8):
        wide_ref[q, channels * 8 :, :] = jnp.zeros(((padded - channels) * 8, cols), jnp.float32)
        wide_ref[q, 0 : channels * 8, :] = value[:, q * 8 : (q + 1) * 8, :].reshape(channels * 8, cols)
    rest = jnp.zeros((LANES - padded, cols), jnp.float32)
    lane = lax.broadcasted_iota(jnp.int32, (cols, LANES), 1)
    sub = lax.broadcasted_iota(jnp.int32, (8, LANES), 0)
    for r in range(rows):
        one = wide_ref[r // 8, pl.ds(r % 8, padded, stride=8), :]
        main = jnp.concatenate([one, rest], axis=0).T
        minus, plus = shifted(main, 0.0, 0.0, sub)
        low, high = pack(minus, main, plus, lane)
        taps_ref[r, :, 0:LANES] = low.astype(jnp.bfloat16)
        taps_ref[r, :, LANES : 2 * LANES] = high.astype(jnp.bfloat16)
    group = w1_raw_ref.shape[1]
    for a in range(3):
        for b in range(3):
            w1_ref[a * 2 * LANES + b * group : a * 2 * LANES + (b + 1) * group, :] = w1_raw_ref[3 * a + b]
        w1_ref[a * 2 * LANES + 3 * group : (a + 1) * 2 * LANES, :] = jnp.zeros(
            (2 * LANES - 3 * group, hid), jnp.bfloat16
        )
    for tap in range(9):
        w2_ref[tap * hid : (tap + 1) * hid, :] = w2_raw_ref[tap].T


def stage(current, w1, w2):
    _, rows, cols = current.shape
    hid = w2.shape[1]
    vmem = pl.BlockSpec(memory_space=pltpu.VMEM)
    return pl.pallas_call(
        stage_kernel,
        out_shape=(
            jax.ShapeDtypeStruct((rows, cols, 2 * LANES), jnp.bfloat16),
            jax.ShapeDtypeStruct((6 * LANES, hid), jnp.bfloat16),
            jax.ShapeDtypeStruct((9 * hid, hid), jnp.bfloat16),
        ),
        in_specs=[vmem] * 3,
        out_specs=(vmem,) * 3,
        scratch_shapes=[pltpu.VMEM((rows // 8, GROUP * 8, cols), jnp.float32)],
        compiler_params=pltpu.CompilerParams(vmem_limit_bytes=16 * 2**20),
        cost_estimate=pl.CostEstimate(flops=2**25, bytes_accessed=2**22, transcendentals=0),
        name="stage",
    )(current, w1, w2)


def prepare_kernel(
    channels, x_ref, fields_ref,
    lat_one_ref, lat_two_ref, lon_one_ref, lon_two_ref, blocks_ref,
    raw_ref, wide_ref, gather_ref, partial_ref, held_ref, extra_ref, lat_ref, lon_ref, first_ref, last_ref,
    x_sem, in_sem, out_sem, extra_sem, halo_sem,
):
    rows, cols = raw_ref.shape[1], raw_ref.shape[2]
    n_lon, n_lat = blocks_ref.shape[0], blocks_ref.shape[1]
    lat, lon = lax.axis_index(LAT), lax.axis_index(LON)

    def load(j):
        part = pl.ds(j * X_PART, min(X_PART, channels - j * X_PART))
        return pltpu.make_async_copy(x_ref.at[part], raw_ref.at[part], x_sem.at[j])

    def get(j):
        return pltpu.make_async_copy(fields_ref.at[0, :, j * cols : (j + 1) * cols], held_ref.at[j], in_sem.at[j])

    def put(j):
        return pltpu.make_async_copy(
            held_ref.at[j].reshape(n_lat, rows, cols), blocks_ref.at[j, :, 0:rows, :], out_sem.at[j]
        )

    def put_extra(j):
        return pltpu.make_async_copy(extra_ref.at[j], blocks_ref.at[j, :, rows : rows + EXTRA, :], extra_sem.at[j])

    halos = [
        pltpu.make_async_copy(lat_ref.at[0], lat_one_ref, halo_sem.at[0]),
        pltpu.make_async_copy(lat_ref.at[1], lat_two_ref, halo_sem.at[1]),
        pltpu.make_async_copy(lon_ref.at[0], lon_one_ref, halo_sem.at[2]),
        pltpu.make_async_copy(lon_ref.at[1], lon_two_ref, halo_sem.at[3]),
    ]
    loads = (channels + X_PART - 1) // X_PART
    for j in range(loads):
        load(j).start()
    for j in range(n_lon):
        get(j).start()
    padded = wide_ref.shape[1] // 8
    for q in range(rows // 8):
        wide_ref[q, channels * 8 :, :] = jnp.zeros(((padded - channels) * 8, cols), jnp.float32)
    partial_ref[:, channels * 8 :, :] = jnp.zeros((2, (padded - channels) * 8, cols), jnp.float32)
    for j in range(loads):
        load(j).wait()
        low, high = j * X_PART, min((j + 1) * X_PART, channels)
        count = high - low
        value = raw_ref[low:high].astype(jnp.float32)
        for q in range(rows // 8):
            wide_ref[q, low * 8 : high * 8, :] = value[:, q * 8 : (q + 1) * 8, :].reshape(count * 8, cols)
        value = value.reshape(count, rows // 8, 8, cols)
        partial_ref[0, low * 8 : high * 8, :] = jnp.sum(value, axis=1).reshape(count * 8, cols)
        partial_ref[1, low * 8 : high * 8, :] = jnp.sum(value * value, axis=1).reshape(count * 8, cols)
    rest = jnp.zeros((LANES - padded, cols), jnp.float32)
    odd_lat = lat % 2 == 1
    odd_lon = lon % 2 == 1
    lane = lax.broadcasted_iota(jnp.int32, (padded, cols), 1)
    columns = jnp.zeros((padded, cols), jnp.float32)
    kept = {}
    for r in range(rows):
        one = wide_ref[r // 8, pl.ds(r % 8, padded, stride=8), :]
        columns = jnp.where(lane // 4 == r, pltpu.roll(one, (2 + 4 * r) % cols, axis=1), columns)
        if r >= 16 and r % 2 == 1:
            get(r // 2 - 8).wait()
            put(r // 2 - 8).start()
        if r in (0, 1, rows - 2, rows - 1):
            kept[r] = jnp.concatenate([one, rest], axis=0).T
    for j in range(2):
        low, high = kept[j], kept[rows - 2 + j]
        lat_ref[0, j] = jnp.where(odd_lat, low, high).astype(jnp.bfloat16)
        lat_ref[1, j] = jnp.where(odd_lat, high, low).astype(jnp.bfloat16)
    halos[0].start()
    halos[1].start()
    gather_ref[...] = jnp.concatenate([columns, rest], axis=0).T
    for j in range(2):
        last_ref[j] = gather_ref[pl.ds(j, rows, stride=4), :]
        first_ref[j] = gather_ref[pl.ds(2 + j, rows, stride=4), :]
    low, high = first_ref[...], last_ref[...]
    lon_ref[0] = jnp.where(odd_lon, low, high).astype(jnp.bfloat16)
    lon_ref[1] = jnp.where(odd_lon, high, low).astype(jnp.bfloat16)
    halos[2].start()
    halos[3].start()

    def parts(which):
        value = partial_ref[which, pl.ds(0, padded, stride=8), :]
        for i in range(1, 8):
            value = value + partial_ref[which, pl.ds(i, padded, stride=8), :]
        value = jnp.sum(jnp.concatenate([value, rest], axis=0).T, axis=0, keepdims=True)
        high = value.astype(jnp.bfloat16).astype(jnp.float32)
        value = value - high
        middle = value.astype(jnp.bfloat16).astype(jnp.float32)
        return [high, middle, value - middle]

    sums = parts(0) + parts(1)
    line = lax.broadcasted_iota(jnp.int32, (1, LANES), 1)

    def extra(down, right):
        cols_ref = last_ref if right > 0 else first_ref
        row = rows - 2 if down > 0 else 0
        near = [cols_ref[j, row : row + 1, :] for j in range(2)]
        far = [cols_ref[j, row + 1 : row + 2, :] for j in range(2)]
        spill = [
            jnp.where(
                jnp.logical_and(line >= SPILL + LANES - channels, line < SPILL + channels),
                pltpu.roll(far[j], SPILL, axis=1), sums[j],
            )
            for j in range(2)
        ]
        both = [jnp.where(line < channels, near[j], pltpu.roll(far[j], channels, axis=1)) for j in range(2)]
        return jnp.concatenate(spill + sums[2:] + both, axis=0).astype(jnp.bfloat16)

    extra_ref[...] = jnp.broadcast_to(extra(1, 1)[None, None], extra_ref.shape)
    for down, right in ((1, -1), (-1, 1), (-1, -1)):
        extra_ref[(lon + n_lon + right) % n_lon, (lat + n_lat + down) % n_lat] = extra(down, right)
    for j in range(n_lon):
        put_extra(j).start()
    for j in range(n_lon):
        put(j).wait()
        put_extra(j).wait()
    for halo in halos:
        halo.wait()


def prepare(current, next_fields, n_lon):
    channels, rows, cols = current.shape
    hbm = pl.BlockSpec(memory_space=pl.ANY)
    height = next_fields.shape[1]
    lat_row = jax.ShapeDtypeStruct((2, cols, LANES), jnp.bfloat16)
    lon_row = jax.ShapeDtypeStruct((2, rows, LANES), jnp.bfloat16)
    return pl.pallas_call(
        functools.partial(prepare_kernel, channels),
        out_shape=(
            lat_row, lat_row, lon_row, lon_row,
            jax.ShapeDtypeStruct((n_lon, height // rows, rows + EXTRA, cols), jnp.bfloat16),
        ),
        in_specs=[hbm, hbm],
        out_specs=(hbm,) * 5,
        scratch_shapes=[
            pltpu.VMEM((channels, rows, cols), jnp.bfloat16),
            pltpu.VMEM((rows // 8, GROUP * 8, cols), jnp.float32),
            pltpu.VMEM((cols, LANES), jnp.float32),
            pltpu.VMEM((2, GROUP * 8, cols), jnp.float32),
            pltpu.VMEM((n_lon, height, cols), jnp.bfloat16),
            pltpu.VMEM((n_lon, height // rows, EXTRA, cols), jnp.bfloat16),
            pltpu.VMEM((2, 2, cols, LANES), jnp.bfloat16),
            pltpu.VMEM((2, 2, rows, LANES), jnp.bfloat16),
            pltpu.VMEM((2, rows, LANES), jnp.float32),
            pltpu.VMEM((2, rows, LANES), jnp.float32),
            pltpu.SemaphoreType.DMA(((channels + X_PART - 1) // X_PART,)),
            pltpu.SemaphoreType.DMA((n_lon,)),
            pltpu.SemaphoreType.DMA((n_lon,)),
            pltpu.SemaphoreType.DMA((n_lon,)),
            pltpu.SemaphoreType.DMA((4,)),
        ],
        compiler_params=pltpu.CompilerParams(vmem_limit_bytes=PREPARE_VMEM),
        cost_estimate=pl.CostEstimate(flops=2**24, bytes_accessed=2**22, transcendentals=0),
        name="prepare",
    )(current, next_fields)


def in_hbm(array):
    return pltpu.with_memory_space_constraint(array, pltpu.HBM)


def pairs(count, periodic):
    near = [(i, i ^ 1) for i in range(count)]
    far = [(i, i + 1 if i % 2 else i - 1) for i in range(count)]
    if periodic:
        return near, [(a, b % count) for a, b in far]
    return near, [(a, b) for a, b in far if 0 <= b < count]


def body(current, next_fields, reader_slot, first_weight, first_bias, second_weight, second_bias):
    channels, rows, cols = current.shape
    n_lat = lax.axis_size(LAT)
    n_lon = lax.axis_size(LON)
    lat_one, lat_two, sent_one, sent_two, blocks = prepare(current, next_fields, n_lon)
    moved = lax.all_to_all(
        blocks.reshape(n_lon * n_lat, rows + EXTRA, cols), LON + LAT, split_axis=0, concat_axis=0, tiled=True
    )
    near, far = pairs(n_lat, False)
    lat_one = lax.ppermute(lat_one, LAT, near)
    lat_two = lax.ppermute(lat_two, LAT, far)
    near, far = pairs(n_lon, True)
    lon_one = lax.ppermute(sent_one, LON, near)
    lon_two = lax.ppermute(sent_two, LON, far)
    w1 = jnp.pad(first_weight.transpose(0, 2, 1), ((0, 0), (0, GROUP - channels), (0, 0)))
    taps, w1, w2 = stage(current, w1, second_weight)
    place = (reader_slot % n_lon) * n_lat + reader_slot // n_lon
    taps, w1, w2 = in_hbm(taps), in_hbm(w1), in_hbm(w2)
    return convs(
        channels, place, taps, lat_one, lat_two, sent_one, sent_two, lon_one, lon_two,
        w1, first_bias[None], w2, second_bias[None], moved,
    )


def solution(mesh):
    split = Mesh(mesh.devices.reshape(4, 2, 2, 2, 4), ("lat_0", "lat_1", "lat_2", "lon_0", "lon_1"))
    return jax.shard_map(
        body,
        mesh=split,
        in_specs=(P(None, LAT, LON), P(LAT + LON, None, None), P(), P(), P(), P(), P()),
        out_specs=(P(None, LAT, LON), P(None, LAT, LON)),
        check_vma=False,
    )
```

```python
import functools

import jax
import jax.numpy as jnp
from jax import lax
from jax.experimental import pallas as pl
from jax.experimental.pallas import tpu as pltpu
from jax.sharding import Mesh
from jax.sharding import PartitionSpec as P

LAT = ("lat_0", "lat_1", "lat_2")
LON = ("lon_0", "lon_1")
LANES = 128
BLOCK = 8
UNIT = 2
EXTRA = 8
X_PART = 24
SPILL = 13
GROUP = 72
PREPARE_VMEM = 16 * 2**20
CONVS_VMEM = 40 * 2**20
GELU_C = 0.7978845608028654


def gelu(v):
    return (0.5 * v) * (1.0 + jnp.tanh(v * (GELU_C + (GELU_C * 0.044715) * (v * v))))


def pack(minus, zero, plus, lanes):
    over = 2 * GROUP - LANES
    turned = pltpu.roll(zero, GROUP, axis=1)
    low = jnp.where(lanes < GROUP, minus, turned)
    high = jnp.where(lanes < over, turned, pltpu.roll(plus, over, axis=1))
    return low, high


def shifted(main, before, after, sub8):
    cols = main.shape[0]
    minus = pltpu.roll(main, 1, axis=0)
    minus = jnp.concatenate([jnp.where(sub8 == 0, before, minus[:8]), minus[8:]], axis=0)
    plus = pltpu.roll(main, cols - 1, axis=0)
    plus = jnp.concatenate([plus[: cols - 8], jnp.where(sub8 == 7, after, plus[cols - 8 :])], axis=0)
    return minus, plus


def conv_kernel(
    channels, rows, cols, hid,
    place_ref, taps_hbm_ref, lat_one_ref, lat_two_ref, sent_one_ref, sent_two_ref, lon_one_ref, lon_two_ref,
    w1_hbm_ref, b1_ref, w2_hbm_ref, b2_ref, moved_ref, out_ref, tile_ref,
    raw_taps_ref, w1_ref, w2_ref, taps_ref, edge_ref, edge_taps_ref, edge_hid_ref, west_ref, mid_ref, east_ref,
    turned_ref, done_ref, sem, take_sem, load_sem,
):
    n_lat, n_lon = lax.axis_size(LAT), lax.axis_size(LON)
    cells = rows * cols * moved_ref.shape[0]
    lat, lon = lax.axis_index(LAT), lax.axis_index(LON)
    first = lat == 0
    last = lat == n_lat - 1
    odd_lat = lat % 2 == 1
    odd_lon = lon % 2 == 1
    lane = lax.broadcasted_iota(jnp.int32, (cols, LANES), 1)
    sub = lax.broadcasted_iota(jnp.int32, (8, LANES), 0)
    lane8 = lax.broadcasted_iota(jnp.int32, (8, LANES), 1)
    sub_hid = lax.broadcasted_iota(jnp.int32, (8, hid), 0)
    group = GROUP
    over = 2 * group - LANES

    def norm(raw):
        return (raw.astype(jnp.float32) - mean) * scale

    def lat_row(row):
        if row < 2:
            return jnp.where(odd_lat, lat_one_ref[row], lat_two_ref[row]), jnp.logical_not(first)
        row = row - rows - 2
        return jnp.where(odd_lat, lat_two_ref[row], lat_one_ref[row]), jnp.logical_not(last)

    def build(row):
        before, after = edge_ref[0, 1, row : row + 1, :], edge_ref[1, 1, row : row + 1, :]
        if 2 <= row < rows + 2:
            raw = raw_taps_ref[row - 2].astype(jnp.float32)
            low = (raw[:, 0:LANES] - mean_low) * scale_low
            high = (raw[:, LANES : 2 * LANES] - mean_high) * scale_high
            head = jnp.where(jnp.logical_and(sub == 0, lane8 < group), before, low[:8])
            tail = jnp.where(
                jnp.logical_and(sub == 7, lane8 >= over), pltpu.roll(after, over, axis=1), high[cols - 8 :]
            )
            low = jnp.concatenate([head, low[8:]], axis=0)
            high = jnp.concatenate([high[: cols - 8], tail], axis=0)
        else:
            raw, keep = lat_row(row)
            main = jnp.where(keep, norm(raw), 0.0)
            minus, plus = shifted(main, before, after, sub)
            low, high = pack(minus, main, plus, lane)
        taps_ref[row, :, 0:LANES] = low.astype(jnp.bfloat16)
        taps_ref[row, :, LANES : 2 * LANES] = high.astype(jnp.bfloat16)

    def corner(down, right):
        there = ((lon + right) % n_lon) * n_lat + (lat + down) % n_lat
        block = moved_ref[there, rows : rows + EXTRA, :].astype(jnp.float32)
        line = lax.broadcasted_iota(jnp.int32, (1, LANES), 1)
        split = LANES - channels
        cells = []
        for j in range(2):
            cells.append(block[6 + j : 7 + j])
        for j in range(2):
            head = pltpu.roll(block[6 + j : 7 + j], LANES - channels, axis=1)
            tail = pltpu.roll(block[j : j + 1], LANES - SPILL, axis=1)
            cells.append(jnp.where(line < split, head, tail))
        return cells

    def edges():
        sides = (
            (odd_lon, lon_one_ref, lon_two_ref, sent_one_ref, sent_two_ref),
            (odd_lon, lon_two_ref, lon_one_ref, sent_two_ref, sent_one_ref),
        )
        keep_top = jnp.logical_not(first)
        keep_bottom = jnp.logical_not(last)
        for side, (odd, one_ref, two_ref, own_one_ref, own_two_ref) in enumerate(sides):
            own_part = 2 if side == 0 else 0
            own = jnp.where(odd, own_one_ref[side], own_two_ref[side])
            edge_ref[side, own_part, 2 : rows + 2, :] = norm(own)
            for row in (0, 1, rows + 2, rows + 3):
                raw, keep = lat_row(row)
                value = norm(raw[0:16] if side == 0 else raw[cols - 16 : cols])
                value = value[0:1] if side == 0 else value[15:16]
                edge_ref[side, own_part, row : row + 1, :] = jnp.where(keep, value, 0.0)
            right = 1 if side == 1 else -1
            top = corner(-1, right)
            bottom = corner(1, right)
            for j in range(2):
                part = j + side
                edge_ref[side, part, 2 : rows + 2, :] = norm(jnp.where(odd, one_ref[j], two_ref[j]))
                for i in range(2):
                    edge_ref[side, part, i : i + 1, :] = jnp.where(keep_top, norm(top[2 * i + j]), 0.0)
                    edge_ref[side, part, rows + 2 + i : rows + 3 + i, :] = jnp.where(
                        keep_bottom, norm(bottom[2 * i + j]), 0.0
                    )
        tall = edge_ref.shape[2]
        for side in range(2):
            for part in range(3):
                edge_ref[side, part, rows + 4 : tall, :] = jnp.zeros((tall - rows - 4, LANES), jnp.float32)

    def edges_hidden():
        tall = edge_ref.shape[2]
        edge_lane = lax.broadcasted_iota(jnp.int32, (tall, LANES), 1)
        hid_row = lax.broadcasted_iota(jnp.int32, (tall - 8, hid), 0)
        hid_outside = jnp.logical_or(
            jnp.logical_and(first, hid_row < 1), jnp.logical_and(last, hid_row >= rows + 1)
        )
        for side in range(2):
            low, high = pack(edge_ref[side, 0], edge_ref[side, 1], edge_ref[side, 2], edge_lane)
            edge_taps_ref[side, :, 0:LANES] = low
            edge_taps_ref[side, :, LANES : 2 * LANES] = high
            stacked = jnp.concatenate(
                [edge_taps_ref[side, a : a + tall - 8, :].astype(jnp.bfloat16) for a in range(3)], axis=1
            )
            value = jnp.dot(stacked, w1_ref[...], preferred_element_type=jnp.float32) + b1_ref[...]
            edge_hid_ref[side] = jnp.where(hid_outside, 0.0, gelu(value))

    def hidden(row, count):
        stacked = jnp.concatenate(
            [taps_ref[row + a : row + a + count].reshape(count * cols, 2 * LANES) for a in range(3)], axis=1
        )
        value = jnp.dot(stacked, w1_ref[...], preferred_element_type=jnp.float32)
        for i in range(count):
            r = row + i
            one = gelu(value[i * cols : (i + 1) * cols] + b1_ref[...])
            if r == 0:
                one = jnp.where(first, 0.0, one)
            elif r == rows + 1:
                one = jnp.where(last, 0.0, one)
            west, east = shifted(one, edge_hid_ref[0, r : r + 1, :], edge_hid_ref[1, r : r + 1, :], sub_hid)
            west_ref[r] = west.astype(jnp.bfloat16)
            mid_ref[r] = one.astype(jnp.bfloat16)
            east_ref[r] = east.astype(jnp.bfloat16)

    def put(t):
        return pltpu.make_async_copy(
            done_ref.at[t], out_ref.at[:, t * BLOCK : (t + 1) * BLOCK, :], sem.at[t]
        )

    def features(u):
        base = u * UNIT
        stacked = jnp.concatenate(
            [
                ref[base + a : base + a + UNIT].reshape(UNIT * cols, hid)
                for a in range(3)
                for ref in (west_ref, mid_ref, east_ref)
            ],
            axis=1,
        )
        value = jnp.dot(stacked, w2_ref[...], preferred_element_type=jnp.float32) + b2_ref[...]
        t, at = base // BLOCK, base % BLOCK
        for i in range(UNIT):
            turned_ref[t % 2, pl.ds(at + i, hid, stride=BLOCK), :] = value[i * cols : (i + 1) * cols].T
        if at + UNIT == BLOCK:
            done_ref[t] = turned_ref[t % 2].reshape(hid, BLOCK, cols).astype(jnp.bfloat16)
            put(t).start()

    steps = rows // BLOCK
    taken = tile_ref.shape[0]

    def load_taps(t):
        low = 0 if t == 0 else t * BLOCK + 2
        part = pl.ds(low, min((t + 1) * BLOCK + 2, rows) - low)
        return pltpu.make_async_copy(taps_hbm_ref.at[part], raw_taps_ref.at[part], load_sem.at[t])

    load_weights = pltpu.make_async_copy(w2_hbm_ref, w2_ref, load_sem.at[steps])
    load_first = pltpu.make_async_copy(w1_hbm_ref, w1_ref, load_sem.at[steps + 1])
    load_taps(0).start()
    load_first.start()
    load_weights.start()
    for t in range(1, steps):
        load_taps(t).start()

    sums = jnp.sum(moved_ref[:, rows : rows + EXTRA, :].astype(jnp.float32), axis=0)
    line = lax.broadcasted_iota(jnp.int32, (1, LANES), 1)
    mean = (sums[0:1] + sums[1:2] + sums[2:3]) / cells
    square = (sums[3:4] + sums[4:5] + sums[5:6]) / cells
    mean = jnp.where(line < channels, mean, 0.0)
    square = jnp.where(line < channels, square, 0.0)
    scale = 1.0 / jnp.sqrt(square - mean * mean + 1e-05)
    scale = jnp.where(line < channels, scale, 0.0)
    mean_low, mean_high = pack(mean, mean, mean, line)
    scale_low, scale_high = pack(scale, scale, scale, line)
    edges()
    load_taps(0).wait()
    for r in range(UNIT + 4):
        build(r)
    load_first.wait()
    edges_hidden()
    hidden(0, UNIT + 2)
    for c in range(taken):
        pltpu.make_async_copy(moved_ref.at[place_ref[c], 0:rows, :], tile_ref.at[c], take_sem).start()
    for t in range(1, steps):
        load_taps(t).wait()
    load_weights.wait()
    units = rows // UNIT

    def more(u):
        if u < units:
            for r in range(u * UNIT + 4, (u + 1) * UNIT + 4):
                build(r)

    more(1)
    for u in range(units):
        more(u + 2)
        if u + 1 < units:
            hidden((u + 1) * UNIT + 2, UNIT)
        features(u)
    pltpu.make_async_copy(moved_ref.at[0:taken, 0:rows, :], tile_ref, take_sem).wait()
    for t in range(steps):
        put(t).wait()


def convs(channels, place, taps, lat_one, lat_two, sent_one, sent_two, lon_one, lon_two, w1, b1, w2, b2, moved):
    rows, cols = taps.shape[0], taps.shape[1]
    hid = w2.shape[1]
    taken = place.shape[0]
    tall = (rows + 4 + 7) // 8 * 8 + 8
    vmem = pl.BlockSpec(memory_space=pltpu.VMEM)
    smem = pl.BlockSpec(memory_space=pltpu.SMEM)
    hbm = pl.BlockSpec(memory_space=pl.ANY)
    flops = 2 * hid * (rows * cols * 9 * hid + (rows + 2) * (cols + 2) * 3 * 256)
    return pl.pallas_call(
        functools.partial(conv_kernel, channels, rows, cols, hid),
        out_shape=(
            jax.ShapeDtypeStruct((hid, rows, cols), jnp.bfloat16),
            jax.ShapeDtypeStruct((taken, rows, cols), jnp.bfloat16),
        ),
        in_specs=[smem, hbm] + [vmem] * 6 + [hbm, vmem, hbm, vmem, vmem],
        out_specs=(hbm, hbm),
        scratch_shapes=[
            pltpu.VMEM((rows, cols, 2 * LANES), jnp.bfloat16),
            pltpu.VMEM((6 * LANES, hid), jnp.bfloat16),
            pltpu.VMEM((9 * hid, hid), jnp.bfloat16),
            pltpu.VMEM((rows + 4, cols, 2 * LANES), jnp.bfloat16),
            pltpu.VMEM((2, 3, tall, LANES), jnp.float32),
            pltpu.VMEM((2, tall, 2 * LANES), jnp.float32),
            pltpu.VMEM((2, tall - 8, hid), jnp.float32),
            pltpu.VMEM((rows + 2, cols, hid), jnp.bfloat16),
            pltpu.VMEM((rows + 2, cols, hid), jnp.bfloat16),
            pltpu.VMEM((rows + 2, cols, hid), jnp.bfloat16),
            pltpu.VMEM((2, hid * BLOCK, cols), jnp.float32),
            pltpu.VMEM((rows // BLOCK, hid, BLOCK, cols), jnp.bfloat16),
            pltpu.SemaphoreType.DMA((rows // BLOCK,)),
            pltpu.SemaphoreType.DMA,
            pltpu.SemaphoreType.DMA((rows // BLOCK + 2,)),
        ],
        compiler_params=pltpu.CompilerParams(vmem_limit_bytes=CONVS_VMEM),
        cost_estimate=pl.CostEstimate(flops=flops, bytes_accessed=8 * 2**20, transcendentals=0),
        name="convs",
    )(place, taps, lat_one, lat_two, sent_one, sent_two, lon_one, lon_two, w1, b1, w2, b2, moved)


def stage_kernel(x_ref, w1_raw_ref, w2_raw_ref, taps_ref, w1_ref, w2_ref, wide_ref):
    channels, rows, cols = x_ref.shape
    hid = w2_ref.shape[1]
    padded = wide_ref.shape[1] // 8
    value = x_ref[...].astype(jnp.float32)
    for q in range(rows // 8):
        wide_ref[q, channels * 8 :, :] = jnp.zeros(((padded - channels) * 8, cols), jnp.float32)
        wide_ref[q, 0 : channels * 8, :] = value[:, q * 8 : (q + 1) * 8, :].reshape(channels * 8, cols)
    rest = jnp.zeros((LANES - padded, cols), jnp.float32)
    lane = lax.broadcasted_iota(jnp.int32, (cols, LANES), 1)
    sub = lax.broadcasted_iota(jnp.int32, (8, LANES), 0)
    for r in range(rows):
        one = wide_ref[r // 8, pl.ds(r % 8, padded, stride=8), :]
        main = jnp.concatenate([one, rest], axis=0).T
        minus, plus = shifted(main, 0.0, 0.0, sub)
        low, high = pack(minus, main, plus, lane)
        taps_ref[r, :, 0:LANES] = low.astype(jnp.bfloat16)
        taps_ref[r, :, LANES : 2 * LANES] = high.astype(jnp.bfloat16)
    group = w1_raw_ref.shape[1]
    for a in range(3):
        for b in range(3):
            w1_ref[a * 2 * LANES + b * group : a * 2 * LANES + (b + 1) * group, :] = w1_raw_ref[3 * a + b]
        w1_ref[a * 2 * LANES + 3 * group : (a + 1) * 2 * LANES, :] = jnp.zeros(
            (2 * LANES - 3 * group, hid), jnp.bfloat16
        )
    for tap in range(9):
        w2_ref[tap * hid : (tap + 1) * hid, :] = w2_raw_ref[tap].T


def stage(current, w1, w2):
    _, rows, cols = current.shape
    hid = w2.shape[1]
    vmem = pl.BlockSpec(memory_space=pltpu.VMEM)
    return pl.pallas_call(
        stage_kernel,
        out_shape=(
            jax.ShapeDtypeStruct((rows, cols, 2 * LANES), jnp.bfloat16),
            jax.ShapeDtypeStruct((6 * LANES, hid), jnp.bfloat16),
            jax.ShapeDtypeStruct((9 * hid, hid), jnp.bfloat16),
        ),
        in_specs=[vmem] * 3,
        out_specs=(vmem,) * 3,
        scratch_shapes=[pltpu.VMEM((rows // 8, GROUP * 8, cols), jnp.float32)],
        compiler_params=pltpu.CompilerParams(vmem_limit_bytes=16 * 2**20),
        cost_estimate=pl.CostEstimate(flops=2**25, bytes_accessed=2**22, transcendentals=0),
        name="stage",
    )(current, w1, w2)


def prepare_kernel(
    channels, x_ref, fields_ref,
    lat_one_ref, lat_two_ref, lon_one_ref, lon_two_ref, blocks_ref,
    raw_ref, wide_ref, gather_ref, partial_ref, held_ref, extra_ref, first_ref, last_ref,
    x_sem, in_sem, out_sem, extra_sem,
):
    rows, cols = raw_ref.shape[1], raw_ref.shape[2]
    n_lon, n_lat = blocks_ref.shape[0], blocks_ref.shape[1]
    lat, lon = lax.axis_index(LAT), lax.axis_index(LON)

    def load(j):
        part = pl.ds(j * X_PART, min(X_PART, channels - j * X_PART))
        return pltpu.make_async_copy(x_ref.at[part], raw_ref.at[part], x_sem.at[j])

    def get(j):
        return pltpu.make_async_copy(fields_ref.at[0, :, j * cols : (j + 1) * cols], held_ref.at[j], in_sem.at[j])

    def put(j):
        return pltpu.make_async_copy(
            held_ref.at[j].reshape(n_lat, rows, cols), blocks_ref.at[j, :, 0:rows, :], out_sem.at[j]
        )

    def put_extra(j):
        return pltpu.make_async_copy(extra_ref.at[j], blocks_ref.at[j, :, rows : rows + EXTRA, :], extra_sem.at[j])

    loads = (channels + X_PART - 1) // X_PART
    for j in range(loads):
        load(j).start()
    for j in range(n_lon):
        get(j).start()
    padded = wide_ref.shape[1] // 8
    for q in range(rows // 8):
        wide_ref[q, channels * 8 :, :] = jnp.zeros(((padded - channels) * 8, cols), jnp.float32)
    partial_ref[:, channels * 8 :, :] = jnp.zeros((2, (padded - channels) * 8, cols), jnp.float32)
    for j in range(loads):
        load(j).wait()
        low, high = j * X_PART, min((j + 1) * X_PART, channels)
        count = high - low
        value = raw_ref[low:high].astype(jnp.float32)
        for q in range(rows // 8):
            wide_ref[q, low * 8 : high * 8, :] = value[:, q * 8 : (q + 1) * 8, :].reshape(count * 8, cols)
        value = value.reshape(count, rows // 8, 8, cols)
        partial_ref[0, low * 8 : high * 8, :] = jnp.sum(value, axis=1).reshape(count * 8, cols)
        partial_ref[1, low * 8 : high * 8, :] = jnp.sum(value * value, axis=1).reshape(count * 8, cols)
    rest = jnp.zeros((LANES - padded, cols), jnp.float32)
    odd_lat = lat % 2 == 1
    odd_lon = lon % 2 == 1

    def row(r):
        return wide_ref[r // 8, pl.ds(r % 8, padded, stride=8), :]

    def parts(which):
        value = partial_ref[which, pl.ds(0, padded, stride=8), :]
        for i in range(1, 8):
            value = value + partial_ref[which, pl.ds(i, padded, stride=8), :]
        value = jnp.sum(jnp.concatenate([value, rest], axis=0).T, axis=0, keepdims=True)
        high = value.astype(jnp.bfloat16).astype(jnp.float32)
        value = value - high
        middle = value.astype(jnp.bfloat16).astype(jnp.float32)
        return [high, middle, value - middle]

    kept = {r: jnp.concatenate([row(r), rest], axis=0).T for r in (0, 1, rows - 2, rows - 1)}
    for j in range(2):
        low, high = kept[j], kept[rows - 2 + j]
        lat_one_ref[j] = jnp.where(odd_lat, low, high).astype(jnp.bfloat16)
        lat_two_ref[j] = jnp.where(odd_lat, high, low).astype(jnp.bfloat16)

    sums = parts(0) + parts(1)
    line = lax.broadcasted_iota(jnp.int32, (1, LANES), 1)

    def extra(down, right):
        col = cols - 2 if right > 0 else 0
        top = rows - 2 if down > 0 else 0
        near = [kept[top][col + j : col + j + 1] for j in range(2)]
        far = [kept[top + 1][col + j : col + j + 1] for j in range(2)]
        spill = [
            jnp.where(
                jnp.logical_and(line >= SPILL + LANES - channels, line < SPILL + channels),
                pltpu.roll(far[j], SPILL, axis=1), sums[j],
            )
            for j in range(2)
        ]
        both = [jnp.where(line < channels, near[j], pltpu.roll(far[j], channels, axis=1)) for j in range(2)]
        return jnp.concatenate(spill + sums[2:] + both, axis=0).astype(jnp.bfloat16)

    extra_ref[...] = jnp.broadcast_to(extra(1, 1)[None, None], extra_ref.shape)
    for down, right in ((1, -1), (-1, 1), (-1, -1)):
        extra_ref[(lon + n_lon + right) % n_lon, (lat + n_lat + down) % n_lat] = extra(down, right)
    for j in range(n_lon):
        put_extra(j).start()
    lane = lax.broadcasted_iota(jnp.int32, (padded, cols), 1)
    columns = jnp.zeros((padded, cols), jnp.float32)
    for r in range(rows):
        columns = jnp.where(lane // 4 == r, pltpu.roll(row(r), (2 + 4 * r) % cols, axis=1), columns)
        if r % 4 == 3:
            get(r // 4).wait()
            put(r // 4).start()
    gather_ref[...] = jnp.concatenate([columns, rest], axis=0).T
    for j in range(2):
        last_ref[j] = gather_ref[pl.ds(j, rows, stride=4), :]
        first_ref[j] = gather_ref[pl.ds(2 + j, rows, stride=4), :]
    low, high = first_ref[...], last_ref[...]
    lon_one_ref[...] = jnp.where(odd_lon, low, high).astype(jnp.bfloat16)
    lon_two_ref[...] = jnp.where(odd_lon, high, low).astype(jnp.bfloat16)
    for j in range(n_lon):
        put(j).wait()
        put_extra(j).wait()


def prepare(current, next_fields, n_lon):
    channels, rows, cols = current.shape
    vmem = pl.BlockSpec(memory_space=pltpu.VMEM)
    hbm = pl.BlockSpec(memory_space=pl.ANY)
    height = next_fields.shape[1]
    lat_row = jax.ShapeDtypeStruct((2, cols, LANES), jnp.bfloat16)
    lon_row = jax.ShapeDtypeStruct((2, rows, LANES), jnp.bfloat16)
    return pl.pallas_call(
        functools.partial(prepare_kernel, channels),
        out_shape=(
            lat_row, lat_row, lon_row, lon_row,
            jax.ShapeDtypeStruct((n_lon, height // rows, rows + EXTRA, cols), jnp.bfloat16),
        ),
        in_specs=[hbm, hbm],
        out_specs=(vmem,) * 4 + (hbm,),
        scratch_shapes=[
            pltpu.VMEM((channels, rows, cols), jnp.bfloat16),
            pltpu.VMEM((rows // 8, GROUP * 8, cols), jnp.float32),
            pltpu.VMEM((cols, LANES), jnp.float32),
            pltpu.VMEM((2, GROUP * 8, cols), jnp.float32),
            pltpu.VMEM((n_lon, height, cols), jnp.bfloat16),
            pltpu.VMEM((n_lon, height // rows, EXTRA, cols), jnp.bfloat16),
            pltpu.VMEM((2, rows, LANES), jnp.float32),
            pltpu.VMEM((2, rows, LANES), jnp.float32),
            pltpu.SemaphoreType.DMA(((channels + X_PART - 1) // X_PART,)),
            pltpu.SemaphoreType.DMA((n_lon,)),
            pltpu.SemaphoreType.DMA((n_lon,)),
            pltpu.SemaphoreType.DMA((n_lon,)),
        ],
        compiler_params=pltpu.CompilerParams(vmem_limit_bytes=PREPARE_VMEM),
        cost_estimate=pl.CostEstimate(flops=2**24, bytes_accessed=2**22, transcendentals=0),
        name="prepare",
    )(current, next_fields)


def in_hbm(array):
    return pltpu.with_memory_space_constraint(array, pltpu.HBM)


def pairs(count, periodic):
    near = [(i, i ^ 1) for i in range(count)]
    far = [(i, i + 1 if i % 2 else i - 1) for i in range(count)]
    if periodic:
        return near, [(a, b % count) for a, b in far]
    return near, [(a, b) for a, b in far if 0 <= b < count]


def body(current, next_fields, reader_slot, first_weight, first_bias, second_weight, second_bias):
    channels, rows, cols = current.shape
    n_lat = lax.axis_size(LAT)
    n_lon = lax.axis_size(LON)
    lat_one, lat_two, sent_one, sent_two, blocks = prepare(in_hbm(current), in_hbm(next_fields), n_lon)
    moved = lax.all_to_all(
        blocks.reshape(n_lon * n_lat, rows + EXTRA, cols), LON + LAT, split_axis=0, concat_axis=0, tiled=True
    )
    near, far = pairs(n_lat, False)
    lat_one = lax.ppermute(lat_one, LAT, near)
    lat_two = lax.ppermute(lat_two, LAT, far)
    near, far = pairs(n_lon, True)
    lon_one = lax.ppermute(sent_one, LON, near)
    lon_two = lax.ppermute(sent_two, LON, far)
    w1 = jnp.pad(first_weight.transpose(0, 2, 1), ((0, 0), (0, GROUP - channels), (0, 0)))
    taps, w1, w2 = stage(current, w1, second_weight)
    place = (reader_slot % n_lon) * n_lat + reader_slot // n_lon
    taps, w1, w2 = in_hbm(taps), in_hbm(w1), in_hbm(w2)
    return convs(
        channels, place, taps, lat_one, lat_two, sent_one, sent_two, lon_one, lon_two,
        w1, first_bias[None], w2, second_bias[None], moved,
    )


def solution(mesh):
    split = Mesh(mesh.devices.reshape(4, 2, 2, 2, 4), ("lat_0", "lat_1", "lat_2", "lon_0", "lon_1"))
    return jax.shard_map(
        body,
        mesh=split,
        in_specs=(P(None, LAT, LON), P(LAT + LON, None, None), P(), P(), P(), P(), P()),
        out_specs=(P(None, LAT, LON), P(None, LAT, LON)),
        check_vma=False,
    )
```

```python
import functools

import jax
import jax.numpy as jnp
from jax import lax
from jax.experimental import pallas as pl
from jax.experimental.pallas import tpu as pltpu
from jax.sharding import Mesh
from jax.sharding import PartitionSpec as P

LAT = ("lat_0", "lat_1", "lat_2")
LON = ("lon_0", "lon_1")
LANES = 128
BLOCK = 8
UNIT = 2
EXTRA = 8
X_PART = 24
SPILL = 13
GROUP = 72
PREPARE_VMEM = 16 * 2**20
CONVS_VMEM = 40 * 2**20
GELU_C = 0.7978845608028654


def gelu(v):
    return (0.5 * v) * (1.0 + jnp.tanh(v * (GELU_C + (GELU_C * 0.044715) * (v * v))))


def pack(minus, zero, plus, lanes):
    over = 2 * GROUP - LANES
    turned = pltpu.roll(zero, GROUP, axis=1)
    low = jnp.where(lanes < GROUP, minus, turned)
    high = jnp.where(lanes < over, turned, pltpu.roll(plus, over, axis=1))
    return low, high


def shifted(main, before, after, sub8):
    cols = main.shape[0]
    minus = pltpu.roll(main, 1, axis=0)
    minus = jnp.concatenate([jnp.where(sub8 == 0, before, minus[:8]), minus[8:]], axis=0)
    plus = pltpu.roll(main, cols - 1, axis=0)
    plus = jnp.concatenate([plus[: cols - 8], jnp.where(sub8 == 7, after, plus[cols - 8 :])], axis=0)
    return minus, plus


def conv_kernel(
    channels, rows, cols, hid,
    place_ref, taps_hbm_ref, lat_one_ref, lat_two_ref, sent_one_ref, sent_two_ref, lon_one_ref, lon_two_ref,
    w1_hbm_ref, b1_ref, w2_raw_ref, b2_ref, moved_ref, out_ref, tile_ref,
    raw_taps_ref, w1_ref, w2_ref, taps_ref, edge_ref, edge_taps_ref, edge_hid_ref, west_ref, mid_ref, east_ref,
    turned_ref, done_ref, sem, take_sem, load_sem,
):
    n_lat, n_lon = lax.axis_size(LAT), lax.axis_size(LON)
    cells = rows * cols * moved_ref.shape[0]
    lat, lon = lax.axis_index(LAT), lax.axis_index(LON)
    first = lat == 0
    last = lat == n_lat - 1
    odd_lat = lat % 2 == 1
    odd_lon = lon % 2 == 1
    lane = lax.broadcasted_iota(jnp.int32, (cols, LANES), 1)
    sub = lax.broadcasted_iota(jnp.int32, (8, LANES), 0)
    lane8 = lax.broadcasted_iota(jnp.int32, (8, LANES), 1)
    sub_hid = lax.broadcasted_iota(jnp.int32, (8, hid), 0)

    def norm(raw):
        return (raw.astype(jnp.float32) - mean) * scale

    def lat_row(row):
        if row < 2:
            return jnp.where(odd_lat, lat_one_ref[row], lat_two_ref[row]), jnp.logical_not(first)
        row = row - rows - 2
        return jnp.where(odd_lat, lat_two_ref[row], lat_one_ref[row]), jnp.logical_not(last)

    def build(row):
        before, after = edge_ref[0, 1, row : row + 1, :], edge_ref[1, 1, row : row + 1, :]
        if 2 <= row < rows + 2:
            main = norm(raw_taps_ref[row - 2])
        else:
            raw, keep = lat_row(row)
            main = jnp.where(keep, norm(raw), 0.0)
        minus, plus = shifted(main, before, after, sub)
        low, high = pack(minus, main, plus, lane)
        taps_ref[row, :, 0:LANES] = low.astype(jnp.bfloat16)
        taps_ref[row, :, LANES : 2 * LANES] = high.astype(jnp.bfloat16)

    def corner(down, right):
        there = ((lon + right) % n_lon) * n_lat + (lat + down) % n_lat
        block = moved_ref[there, rows : rows + EXTRA, :].astype(jnp.float32)
        line = lax.broadcasted_iota(jnp.int32, (1, LANES), 1)
        split = LANES - channels
        cells = []
        for j in range(2):
            cells.append(block[6 + j : 7 + j])
        for j in range(2):
            head = pltpu.roll(block[6 + j : 7 + j], LANES - channels, axis=1)
            tail = pltpu.roll(block[j : j + 1], LANES - SPILL, axis=1)
            cells.append(jnp.where(line < split, head, tail))
        return cells

    def edges():
        sides = (
            (odd_lon, lon_one_ref, lon_two_ref, sent_one_ref, sent_two_ref),
            (odd_lon, lon_two_ref, lon_one_ref, sent_two_ref, sent_one_ref),
        )
        keep_top = jnp.logical_not(first)
        keep_bottom = jnp.logical_not(last)
        for side, (odd, one_ref, two_ref, own_one_ref, own_two_ref) in enumerate(sides):
            own_part = 2 if side == 0 else 0
            own = jnp.where(odd, own_one_ref[side], own_two_ref[side])
            edge_ref[side, own_part, 2 : rows + 2, :] = norm(own)
            for row in (0, 1, rows + 2, rows + 3):
                raw, keep = lat_row(row)
                value = norm(raw[0:16] if side == 0 else raw[cols - 16 : cols])
                value = value[0:1] if side == 0 else value[15:16]
                edge_ref[side, own_part, row : row + 1, :] = jnp.where(keep, value, 0.0)
            right = 1 if side == 1 else -1
            top = corner(-1, right)
            bottom = corner(1, right)
            for j in range(2):
                part = j + side
                edge_ref[side, part, 2 : rows + 2, :] = norm(jnp.where(odd, one_ref[j], two_ref[j]))
                for i in range(2):
                    edge_ref[side, part, i : i + 1, :] = jnp.where(keep_top, norm(top[2 * i + j]), 0.0)
                    edge_ref[side, part, rows + 2 + i : rows + 3 + i, :] = jnp.where(
                        keep_bottom, norm(bottom[2 * i + j]), 0.0
                    )
        tall = edge_ref.shape[2]
        for side in range(2):
            for part in range(3):
                edge_ref[side, part, rows + 4 : tall, :] = jnp.zeros((tall - rows - 4, LANES), jnp.float32)

    def edges_hidden():
        tall = edge_ref.shape[2]
        edge_lane = lax.broadcasted_iota(jnp.int32, (tall, LANES), 1)
        hid_row = lax.broadcasted_iota(jnp.int32, (tall - 8, hid), 0)
        hid_outside = jnp.logical_or(
            jnp.logical_and(first, hid_row < 1), jnp.logical_and(last, hid_row >= rows + 1)
        )
        for side in range(2):
            low, high = pack(edge_ref[side, 0], edge_ref[side, 1], edge_ref[side, 2], edge_lane)
            edge_taps_ref[side, :, 0:LANES] = low
            edge_taps_ref[side, :, LANES : 2 * LANES] = high
            stacked = jnp.concatenate(
                [edge_taps_ref[side, a : a + tall - 8, :].astype(jnp.bfloat16) for a in range(3)], axis=1
            )
            value = jnp.dot(stacked, w1_ref[...], preferred_element_type=jnp.float32) + b1_ref[...]
            edge_hid_ref[side] = jnp.where(hid_outside, 0.0, gelu(value))

    def hidden(row, count):
        stacked = jnp.concatenate(
            [taps_ref[row + a : row + a + count].reshape(count * cols, 2 * LANES) for a in range(3)], axis=1
        )
        value = jnp.dot(stacked, w1_ref[...], preferred_element_type=jnp.float32)
        for i in range(count):
            r = row + i
            one = gelu(value[i * cols : (i + 1) * cols] + b1_ref[...])
            if r == 0:
                one = jnp.where(first, 0.0, one)
            elif r == rows + 1:
                one = jnp.where(last, 0.0, one)
            west, east = shifted(one, edge_hid_ref[0, r : r + 1, :], edge_hid_ref[1, r : r + 1, :], sub_hid)
            west_ref[r] = west.astype(jnp.bfloat16)
            mid_ref[r] = one.astype(jnp.bfloat16)
            east_ref[r] = east.astype(jnp.bfloat16)

    def put(t):
        return pltpu.make_async_copy(
            done_ref.at[t], out_ref.at[:, t * BLOCK : (t + 1) * BLOCK, :], sem.at[t]
        )

    def features(u):
        base = u * UNIT
        stacked = jnp.concatenate(
            [
                ref[base + a : base + a + UNIT].reshape(UNIT * cols, hid)
                for a in range(3)
                for ref in (west_ref, mid_ref, east_ref)
            ],
            axis=1,
        )
        value = jnp.dot(stacked, w2_ref[...], preferred_element_type=jnp.float32) + b2_ref[...]
        t, at = base // BLOCK, base % BLOCK
        for i in range(UNIT):
            turned_ref[t % 2, pl.ds(at + i, hid, stride=BLOCK), :] = value[i * cols : (i + 1) * cols].T
        if at + UNIT == BLOCK:
            done_ref[t] = turned_ref[t % 2].reshape(hid, BLOCK, cols).astype(jnp.bfloat16)
            put(t).start()

    steps = rows // BLOCK
    taken = tile_ref.shape[0]

    def load_taps(t):
        low = 0 if t == 0 else t * BLOCK + 2
        part = pl.ds(low, min((t + 1) * BLOCK + 2, rows) - low)
        return pltpu.make_async_copy(taps_hbm_ref.at[part], raw_taps_ref.at[part], load_sem.at[t])

    load_first = pltpu.make_async_copy(w1_hbm_ref, w1_ref, load_sem.at[steps + 1])
    load_taps(0).start()
    load_first.start()
    for t in range(1, steps):
        load_taps(t).start()

    sums = jnp.sum(moved_ref[:, rows : rows + EXTRA, :].astype(jnp.float32), axis=0)
    line = lax.broadcasted_iota(jnp.int32, (1, LANES), 1)
    mean = (sums[0:1] + sums[1:2] + sums[2:3]) / cells
    square = (sums[3:4] + sums[4:5] + sums[5:6]) / cells
    mean = jnp.where(line < channels, mean, 0.0)
    square = jnp.where(line < channels, square, 0.0)
    scale = 1.0 / jnp.sqrt(square - mean * mean + 1e-05)
    scale = jnp.where(line < channels, scale, 0.0)
    mean_low, mean_high = pack(mean, mean, mean, line)
    scale_low, scale_high = pack(scale, scale, scale, line)
    edges()
    load_taps(0).wait()
    load_first.wait()
    for t in range(1, steps):
        load_taps(t).wait()
    for r in range(UNIT + 4):
        build(r)
    edges_hidden()
    hidden(0, UNIT + 2)
    for tap in range(9):
        w2_ref[tap * hid : (tap + 1) * hid, :] = w2_raw_ref[tap].T
    for c in range(taken):
        pltpu.make_async_copy(moved_ref.at[place_ref[c], 0:rows, :], tile_ref.at[c], take_sem).start()
    units = rows // UNIT

    def more(u):
        if u < units:
            for r in range(u * UNIT + 4, (u + 1) * UNIT + 4):
                build(r)

    more(1)
    for u in range(units):
        more(u + 2)
        if u + 1 < units:
            hidden((u + 1) * UNIT + 2, UNIT)
        features(u)
    pltpu.make_async_copy(moved_ref.at[0:taken, 0:rows, :], tile_ref, take_sem).wait()
    for t in range(steps):
        put(t).wait()


def convs(channels, place, taps, lat_one, lat_two, sent_one, sent_two, lon_one, lon_two, w1, b1, w2, b2, moved):
    rows, cols = taps.shape[0], taps.shape[1]
    hid = w2.shape[1]
    taken = place.shape[0]
    tall = (rows + 4 + 7) // 8 * 8 + 8
    vmem = pl.BlockSpec(memory_space=pltpu.VMEM)
    smem = pl.BlockSpec(memory_space=pltpu.SMEM)
    hbm = pl.BlockSpec(memory_space=pl.ANY)
    flops = 2 * hid * (rows * cols * 9 * hid + (rows + 2) * (cols + 2) * 3 * 256)
    return pl.pallas_call(
        functools.partial(conv_kernel, channels, rows, cols, hid),
        out_shape=(
            jax.ShapeDtypeStruct((hid, rows, cols), jnp.bfloat16),
            jax.ShapeDtypeStruct((taken, rows, cols), jnp.bfloat16),
        ),
        in_specs=[smem, hbm] + [vmem] * 6 + [hbm] + [vmem] * 4,
        out_specs=(hbm, hbm),
        scratch_shapes=[
            pltpu.VMEM((rows, cols, LANES), jnp.bfloat16),
            pltpu.VMEM((6 * LANES, hid), jnp.bfloat16),
            pltpu.VMEM((9 * hid, hid), jnp.bfloat16),
            pltpu.VMEM((rows + 4, cols, 2 * LANES), jnp.bfloat16),
            pltpu.VMEM((2, 3, tall, LANES), jnp.float32),
            pltpu.VMEM((2, tall, 2 * LANES), jnp.float32),
            pltpu.VMEM((2, tall - 8, hid), jnp.float32),
            pltpu.VMEM((rows + 2, cols, hid), jnp.bfloat16),
            pltpu.VMEM((rows + 2, cols, hid), jnp.bfloat16),
            pltpu.VMEM((rows + 2, cols, hid), jnp.bfloat16),
            pltpu.VMEM((2, hid * BLOCK, cols), jnp.float32),
            pltpu.VMEM((rows // BLOCK, hid, BLOCK, cols), jnp.bfloat16),
            pltpu.SemaphoreType.DMA((rows // BLOCK,)),
            pltpu.SemaphoreType.DMA,
            pltpu.SemaphoreType.DMA((rows // BLOCK + 2,)),
        ],
        compiler_params=pltpu.CompilerParams(vmem_limit_bytes=CONVS_VMEM),
        cost_estimate=pl.CostEstimate(flops=flops, bytes_accessed=8 * 2**20, transcendentals=0),
        name="convs",
    )(place, taps, lat_one, lat_two, sent_one, sent_two, lon_one, lon_two, w1, b1, w2, b2, moved)


def stage_kernel(x_ref, w1_raw_ref, taps_ref, w1_ref, wide_ref):
    channels, rows, cols = x_ref.shape
    hid = w1_ref.shape[1]
    padded = wide_ref.shape[1] // 8
    value = x_ref[...].astype(jnp.float32)
    for q in range(rows // 8):
        wide_ref[q, channels * 8 :, :] = jnp.zeros(((padded - channels) * 8, cols), jnp.float32)
        wide_ref[q, 0 : channels * 8, :] = value[:, q * 8 : (q + 1) * 8, :].reshape(channels * 8, cols)
    rest = jnp.zeros((LANES - padded, cols), jnp.float32)
    lane = lax.broadcasted_iota(jnp.int32, (cols, LANES), 1)
    sub = lax.broadcasted_iota(jnp.int32, (8, LANES), 0)
    for r in range(rows):
        one = wide_ref[r // 8, pl.ds(r % 8, padded, stride=8), :]
        main = jnp.concatenate([one, rest], axis=0).T
        taps_ref[r] = main.astype(jnp.bfloat16)
    group = w1_raw_ref.shape[1]
    for a in range(3):
        for b in range(3):
            w1_ref[a * 2 * LANES + b * group : a * 2 * LANES + (b + 1) * group, :] = w1_raw_ref[3 * a + b]
        w1_ref[a * 2 * LANES + 3 * group : (a + 1) * 2 * LANES, :] = jnp.zeros(
            (2 * LANES - 3 * group, hid), jnp.bfloat16
        )


def stage(current, w1):
    _, rows, cols = current.shape
    hid = w1.shape[2]
    vmem = pl.BlockSpec(memory_space=pltpu.VMEM)
    return pl.pallas_call(
        stage_kernel,
        out_shape=(
            jax.ShapeDtypeStruct((rows, cols, LANES), jnp.bfloat16),
            jax.ShapeDtypeStruct((6 * LANES, hid), jnp.bfloat16),
        ),
        in_specs=[vmem] * 2,
        out_specs=(vmem,) * 2,
        scratch_shapes=[pltpu.VMEM((rows // 8, GROUP * 8, cols), jnp.float32)],
        compiler_params=pltpu.CompilerParams(vmem_limit_bytes=16 * 2**20),
        cost_estimate=pl.CostEstimate(flops=2**25, bytes_accessed=2**22, transcendentals=0),
        name="stage",
    )(current, w1)


def prepare_kernel(
    channels, x_ref, fields_ref,
    lat_one_ref, lat_two_ref, lon_one_ref, lon_two_ref, blocks_ref,
    raw_ref, wide_ref, gather_ref, partial_ref, held_ref, extra_ref, first_ref, last_ref,
    x_sem, in_sem, out_sem, extra_sem,
):
    rows, cols = raw_ref.shape[1], raw_ref.shape[2]
    n_lon, n_lat = blocks_ref.shape[0], blocks_ref.shape[1]
    lat, lon = lax.axis_index(LAT), lax.axis_index(LON)

    def load(j):
        part = pl.ds(j * X_PART, min(X_PART, channels - j * X_PART))
        return pltpu.make_async_copy(x_ref.at[part], raw_ref.at[part], x_sem.at[j])

    def get(j):
        return pltpu.make_async_copy(fields_ref.at[0, :, j * cols : (j + 1) * cols], held_ref.at[j], in_sem.at[j])

    def put(j):
        return pltpu.make_async_copy(
            held_ref.at[j].reshape(n_lat, rows, cols), blocks_ref.at[j, :, 0:rows, :], out_sem.at[j]
        )

    def put_extra(j):
        return pltpu.make_async_copy(extra_ref.at[j], blocks_ref.at[j, :, rows : rows + EXTRA, :], extra_sem.at[j])

    loads = (channels + X_PART - 1) // X_PART
    for j in range(loads):
        load(j).start()
    for j in range(n_lon):
        get(j).start()
    padded = wide_ref.shape[1] // 8
    for q in range(rows // 8):
        wide_ref[q, channels * 8 :, :] = jnp.zeros(((padded - channels) * 8, cols), jnp.float32)
    partial_ref[:, channels * 8 :, :] = jnp.zeros((2, (padded - channels) * 8, cols), jnp.float32)
    for j in range(loads):
        load(j).wait()
        low, high = j * X_PART, min((j + 1) * X_PART, channels)
        count = high - low
        value = raw_ref[low:high].astype(jnp.float32)
        for q in range(rows // 8):
            wide_ref[q, low * 8 : high * 8, :] = value[:, q * 8 : (q + 1) * 8, :].reshape(count * 8, cols)
        value = value.reshape(count, rows // 8, 8, cols)
        partial_ref[0, low * 8 : high * 8, :] = jnp.sum(value, axis=1).reshape(count * 8, cols)
        partial_ref[1, low * 8 : high * 8, :] = jnp.sum(value * value, axis=1).reshape(count * 8, cols)
    rest = jnp.zeros((LANES - padded, cols), jnp.float32)
    odd_lat = lat % 2 == 1
    odd_lon = lon % 2 == 1

    def row(r):
        return wide_ref[r // 8, pl.ds(r % 8, padded, stride=8), :]

    def parts(which):
        value = partial_ref[which, pl.ds(0, padded, stride=8), :]
        for i in range(1, 8):
            value = value + partial_ref[which, pl.ds(i, padded, stride=8), :]
        value = jnp.sum(jnp.concatenate([value, rest], axis=0).T, axis=0, keepdims=True)
        high = value.astype(jnp.bfloat16).astype(jnp.float32)
        value = value - high
        middle = value.astype(jnp.bfloat16).astype(jnp.float32)
        return [high, middle, value - middle]

    kept = {r: jnp.concatenate([row(r), rest], axis=0).T for r in (0, 1, rows - 2, rows - 1)}
    for j in range(2):
        low, high = kept[j], kept[rows - 2 + j]
        lat_one_ref[j] = jnp.where(odd_lat, low, high).astype(jnp.bfloat16)
        lat_two_ref[j] = jnp.where(odd_lat, high, low).astype(jnp.bfloat16)

    sums = parts(0) + parts(1)
    line = lax.broadcasted_iota(jnp.int32, (1, LANES), 1)

    def extra(down, right):
        col = cols - 2 if right > 0 else 0
        top = rows - 2 if down > 0 else 0
        near = [kept[top][col + j : col + j + 1] for j in range(2)]
        far = [kept[top + 1][col + j : col + j + 1] for j in range(2)]
        spill = [
            jnp.where(
                jnp.logical_and(line >= SPILL + LANES - channels, line < SPILL + channels),
                pltpu.roll(far[j], SPILL, axis=1), sums[j],
            )
            for j in range(2)
        ]
        both = [jnp.where(line < channels, near[j], pltpu.roll(far[j], channels, axis=1)) for j in range(2)]
        return jnp.concatenate(spill + sums[2:] + both, axis=0).astype(jnp.bfloat16)

    extra_ref[...] = jnp.broadcast_to(extra(1, 1)[None, None], extra_ref.shape)
    for down, right in ((1, -1), (-1, 1), (-1, -1)):
        extra_ref[(lon + n_lon + right) % n_lon, (lat + n_lat + down) % n_lat] = extra(down, right)
    for j in range(n_lon):
        put_extra(j).start()
    lane = lax.broadcasted_iota(jnp.int32, (padded, cols), 1)
    columns = jnp.zeros((padded, cols), jnp.float32)
    for r in range(rows):
        columns = jnp.where(lane // 4 == r, pltpu.roll(row(r), (2 + 4 * r) % cols, axis=1), columns)
        if r % 4 == 3:
            get(r // 4).wait()
            put(r // 4).start()
    gather_ref[...] = jnp.concatenate([columns, rest], axis=0).T
    for j in range(2):
        last_ref[j] = gather_ref[pl.ds(j, rows, stride=4), :]
        first_ref[j] = gather_ref[pl.ds(2 + j, rows, stride=4), :]
    low, high = first_ref[...], last_ref[...]
    lon_one_ref[...] = jnp.where(odd_lon, low, high).astype(jnp.bfloat16)
    lon_two_ref[...] = jnp.where(odd_lon, high, low).astype(jnp.bfloat16)
    for j in range(n_lon):
        put(j).wait()
        put_extra(j).wait()


def prepare(current, next_fields, n_lon):
    channels, rows, cols = current.shape
    vmem = pl.BlockSpec(memory_space=pltpu.VMEM)
    hbm = pl.BlockSpec(memory_space=pl.ANY)
    height = next_fields.shape[1]
    lat_row = jax.ShapeDtypeStruct((2, cols, LANES), jnp.bfloat16)
    lon_row = jax.ShapeDtypeStruct((2, rows, LANES), jnp.bfloat16)
    return pl.pallas_call(
        functools.partial(prepare_kernel, channels),
        out_shape=(
            lat_row, lat_row, lon_row, lon_row,
            jax.ShapeDtypeStruct((n_lon, height // rows, rows + EXTRA, cols), jnp.bfloat16),
        ),
        in_specs=[hbm, hbm],
        out_specs=(vmem,) * 4 + (hbm,),
        scratch_shapes=[
            pltpu.VMEM((channels, rows, cols), jnp.bfloat16),
            pltpu.VMEM((rows // 8, GROUP * 8, cols), jnp.float32),
            pltpu.VMEM((cols, LANES), jnp.float32),
            pltpu.VMEM((2, GROUP * 8, cols), jnp.float32),
            pltpu.VMEM((n_lon, height, cols), jnp.bfloat16),
            pltpu.VMEM((n_lon, height // rows, EXTRA, cols), jnp.bfloat16),
            pltpu.VMEM((2, rows, LANES), jnp.float32),
            pltpu.VMEM((2, rows, LANES), jnp.float32),
            pltpu.SemaphoreType.DMA(((channels + X_PART - 1) // X_PART,)),
            pltpu.SemaphoreType.DMA((n_lon,)),
            pltpu.SemaphoreType.DMA((n_lon,)),
            pltpu.SemaphoreType.DMA((n_lon,)),
        ],
        compiler_params=pltpu.CompilerParams(vmem_limit_bytes=PREPARE_VMEM),
        cost_estimate=pl.CostEstimate(flops=2**24, bytes_accessed=2**22, transcendentals=0),
        name="prepare",
    )(current, next_fields)


def in_hbm(array):
    return pltpu.with_memory_space_constraint(array, pltpu.HBM)


def pairs(count, periodic):
    near = [(i, i ^ 1) for i in range(count)]
    far = [(i, i + 1 if i % 2 else i - 1) for i in range(count)]
    if periodic:
        return near, [(a, b % count) for a, b in far]
    return near, [(a, b) for a, b in far if 0 <= b < count]


def body(current, next_fields, reader_slot, first_weight, first_bias, second_weight, second_bias):
    channels, rows, cols = current.shape
    n_lat = lax.axis_size(LAT)
    n_lon = lax.axis_size(LON)
    lat_one, lat_two, sent_one, sent_two, blocks = prepare(in_hbm(current), in_hbm(next_fields), n_lon)
    moved = lax.all_to_all(
        blocks.reshape(n_lon * n_lat, rows + EXTRA, cols), LON + LAT, split_axis=0, concat_axis=0, tiled=True
    )
    near, far = pairs(n_lat, False)
    lat_one = lax.ppermute(lat_one, LAT, near)
    lat_two = lax.ppermute(lat_two, LAT, far)
    near, far = pairs(n_lon, True)
    lon_one = lax.ppermute(sent_one, LON, near)
    lon_two = lax.ppermute(sent_two, LON, far)
    w1 = jnp.pad(first_weight.transpose(0, 2, 1), ((0, 0), (0, GROUP - channels), (0, 0)))
    taps, w1 = stage(current, w1)
    place = (reader_slot % n_lon) * n_lat + reader_slot // n_lon
    taps, w1 = in_hbm(taps), in_hbm(w1)
    return convs(
        channels, place, taps, lat_one, lat_two, sent_one, sent_two, lon_one, lon_two,
        w1, first_bias[None], second_weight, second_bias[None], moved,
    )


def solution(mesh):
    split = Mesh(mesh.devices.reshape(4, 2, 2, 2, 4), ("lat_0", "lat_1", "lat_2", "lon_0", "lon_1"))
    return jax.shard_map(
        body,
        mesh=split,
        in_specs=(P(None, LAT, LON), P(LAT + LON, None, None), P(), P(), P(), P(), P()),
        out_specs=(P(None, LAT, LON), P(None, LAT, LON)),
        check_vma=False,
    )
```
